512 devices in a mesh: section: 4 (over y_lo), row: 16 (over z, core), col: 8 (over y_hi, x).
Axes of the slice: x: 4, y: 8 (y_hi: 2, y_lo: 4; y = y_hi * 4 + y_lo), z: 8, core: 2. Of those that a mesh axis runs over, the one named last changes fastest.
Arguments:
- section_input: bfloat16 [4, 2, 128, 128, 128], P('section', None, 'row', 'col'), may hold values from -6 to 6
- first_pre: bfloat16 [4, 2, 128, 128, 128], P('section', None, 'row', 'col'), may hold values from -6 to 6
- second_pre: bfloat16 [4, 2, 128, 128, 128], P('section', None, 'row', 'col'), may hold values from -6 to 6
- out_grad: bfloat16 [2, 128, 128, 128], P(None, 'row', 'col'), may hold values from -6 to 6
- kernels: bfloat16 [4, 2, 3, 3, 128, 128], P('section'), may hold values from -0.1875 to 0.1875
- bn_scale: float32 [4, 2, 128], P('section'), may hold values from 0.5 to 2
- bn_shift: float32 [4, 2, 128], P('section'), may hold values from -3 to 3
Outputs:
- input_grad: bfloat16 [4, 2, 128, 128, 128], P('section', None, 'row', 'col')
- filter_grad: float32 [4, 2, 3, 3, 128, 128], P('section')
The draws below stay inside these ranges and needn't reach their ends.
All inputs are finite; a program needn't handle non-finite values.
Results may differ from the reference program's by a relative error of at most 0.013.
Values may be sent and summed in bfloat16 or wider, within the bound.
No kernel may reach another device: no remote copies, remote signals or barrier semaphores. Data moves between devices by JAX's collectives and lax.ppermute only.
A program may use at most 64 MiB of HBM per device.

```python
import math
import jax
import jax.numpy as jnp
from jax import lax

CHANNELS = 128
MICRO = 2
SECTIONS = 4
IMG_ROWS = 128
IMG_COLS = 128


def shard_levels(own_key, extent, shards, smallest, high):
    def one(dim, shards_of):
        steps = jax.random.uniform(jax.random.fold_in(jax.random.fold_in(own_key, 6), dim), (shards_of,), jnp.float32, smallest / len(shards), high / len(shards))
        return jnp.repeat(jnp.exp(steps), extent[dim] // shards_of).reshape((-1,) + (1,) * (len(extent) - dim - 1))

    factor_of = one(*shards[0])
    for cut in shards[1:]:
        factor_of = factor_of * one(*cut)
    return factor_of


def normal_values(key, dims, scale, bound, cuts=(), dtype=jnp.bfloat16):
    drawn = jax.random.normal(key, dims, jnp.float32) * scale
    if len(cuts) > 0:
        drawn = shard_levels(key, dims, cuts, -0.22, 0.18) * drawn
    return jnp.clip(drawn, min=-bound, max=bound).astype(dtype)


def setup_inputs(seed: int = 0) -> dict:
    arg_keys = jax.random.split(jax.random.key(seed), 8)
    return {
        "section_input": normal_values(arg_keys[0], (SECTIONS, MICRO, IMG_ROWS, IMG_COLS, CHANNELS), 1.0, 6.0, ((0, 4), (2, 16), (3, 8))),
        "first_pre": normal_values(arg_keys[1], (SECTIONS, MICRO, IMG_ROWS, IMG_COLS, CHANNELS), 1.0, 6.0, ((0, 4), (2, 16), (3, 8))),
        "second_pre": normal_values(arg_keys[2], (SECTIONS, MICRO, IMG_ROWS, IMG_COLS, CHANNELS), 1.0, 6.0, ((0, 4), (2, 16), (3, 8))),
        "out_grad": normal_values(arg_keys[3], (MICRO, IMG_ROWS, IMG_COLS, CHANNELS), 1.0, 6.0, ((1, 16), (2, 8))),
        "kernels": normal_values(arg_keys[4], (SECTIONS, 2, 3, 3, CHANNELS, CHANNELS), (9 * CHANNELS) ** -0.5, 0.1875, ((0, 4),)),
        "bn_scale": jnp.clip(jnp.exp(math.log(2.0) - 1.3862944 * jax.random.uniform(arg_keys[5], (SECTIONS, 2, CHANNELS), jnp.float32) ** shard_levels(arg_keys[5], (SECTIONS, 2, CHANNELS), ((0, 4),), -0.2, 0.2)), 0.5, 2.0),
        "bn_shift": normal_values(arg_keys[6], (SECTIONS, 2, CHANNELS), 0.5, 3.0, ((0, 4),), jnp.float32),
    }


def padded_tile(field):
    return jnp.pad(field, ((1, 1), (1, 1), (0, 0)))

def correlate(padded, kernel):
    result = lax.conv_general_dilated(padded[None], kernel, (1, 1), 'VALID', dimension_numbers=('NHWC', 'HWIO', 'NHWC'), preferred_element_type=jnp.float32)
    return result[0]

def flip_kernel(kernel):
    return jnp.transpose(jnp.flip(kernel, (0, 1)), (0, 1, 3, 2))

def kernel_grad(padded, gradient):
    rows_here, cols_here = (gradient.shape[0], gradient.shape[1])
    pieces = []
    for row_off in range(3):
        for col_off in range(3):
            window = padded[row_off:row_off + rows_here, col_off:col_off + cols_here]
            pieces.append(jnp.einsum('hwc,hwd->cd', window, gradient, preferred_element_type=jnp.float32))
    return jnp.stack(pieces).reshape(3, 3, gradient.shape[2], gradient.shape[2])

def unit_backward(inputs, first_pre, second_pre, incoming, kernel, scales, shifts):
    first_norm = scales[0] * first_pre.astype(jnp.float32) + shifts[0]
    first_act = jnp.maximum(first_norm, 0.0).astype(jnp.bfloat16)
    second_norm = scales[1] * second_pre.astype(jnp.float32) + shifts[1]
    masked = jnp.where(second_norm + inputs.astype(jnp.float32) > 0, incoming.astype(jnp.float32), 0.0)
    second_grad = (scales[1] * masked).astype(jnp.bfloat16)
    act_grad = correlate(padded_tile(second_grad), flip_kernel(kernel[1]))
    first_grad = (scales[0] * jnp.where(first_norm > 0, act_grad, 0.0)).astype(jnp.bfloat16)
    input_grad = (masked + correlate(padded_tile(first_grad), flip_kernel(kernel[0]))).astype(jnp.bfloat16)
    grads = jnp.stack([kernel_grad(padded_tile(inputs), first_grad), kernel_grad(padded_tile(first_act), second_grad)])
    return (input_grad, grads)

def reference(section_input, first_pre, second_pre, out_grad, kernels, bn_scale, bn_shift):
    outputs = [[None] * MICRO for _ in range(SECTIONS)]
    filters = [jnp.zeros((2, 3, 3, CHANNELS, CHANNELS), jnp.float32) for _ in range(SECTIONS)]
    for micro_index in range(MICRO):
        incoming = out_grad[micro_index]
        for section_index in reversed(range(SECTIONS)):
            incoming, grads = unit_backward(section_input[section_index, micro_index], first_pre[section_index, micro_index], second_pre[section_index, micro_index], incoming, kernels[section_index], bn_scale[section_index], bn_shift[section_index])
            outputs[section_index][micro_index] = incoming
            filters[section_index] = filters[section_index] + grads
    factor = 1.0 / jnp.sqrt(jnp.float32(MICRO * IMG_ROWS * IMG_COLS))
    input_grad = jnp.stack([jnp.stack(column) for column in outputs])
    filter_grad = jnp.stack(filters) * factor
    return (input_grad, filter_grad)
```

```python
import jax
import jax.numpy as jnp
from jax import lax
from jax.sharding import Mesh
from jax.sharding import PartitionSpec as P

ROW = ("row_0", "row_1")
COL = ("col_0", "col_1")
NEAR = ("row_1", "col_1")
FAR = ("row_0", "col_0")


def with_halo(cells, axis, dim, width):
    count = lax.axis_size(axis)
    size = cells.shape[dim]
    head = lax.slice_in_dim(cells, 0, width, axis=dim)
    tail = lax.slice_in_dim(cells, size - width, size, axis=dim)
    before = lax.ppermute(tail, axis, [(i, i + 1) for i in range(count - 1)])
    after = lax.ppermute(head, axis, [(i + 1, i) for i in range(count - 1)])
    return jnp.concatenate([before, cells, after], axis=dim)


def crop(field, cut):
    if cut == 0:
        return field
    return field[:, cut:-cut, cut:-cut]


def correlate(padded, kernel):
    return lax.conv_general_dilated(
        padded,
        kernel,
        (1, 1),
        "VALID",
        dimension_numbers=("NHWC", "HWIO", "NHWC"),
        preferred_element_type=jnp.float32,
    )


def flip_kernel(kernel):
    return jnp.transpose(jnp.flip(kernel, (0, 1)), (0, 1, 3, 2))


def kernel_grad(cells, padded):
    rows_here, cols_here = (cells.shape[1], cells.shape[2])
    windows = jnp.stack(
        [
            padded[:, 2 - i : 2 - i + rows_here, 2 - j : 2 - j + cols_here]
            for i in range(3)
            for j in range(3)
        ]
    )
    return jnp.einsum("mhwc,kmhwd->kcd", cells, windows, preferred_element_type=jnp.float32)


def sum_of_blocks(blocks, axes):
    parts = lax.all_to_all(blocks, axes, 0, 0, tiled=True)
    return jnp.sum(parts.astype(jnp.float32), axis=0)


def copies(block, axes):
    count = lax.axis_size(axes)
    return lax.all_to_all(jnp.broadcast_to(block[None], (count, *block.shape)), axes, 0, 0, tiled=True)


def total_of(x, factor):
    near, far = (lax.axis_size(NEAR), lax.axis_size(FAR))
    width = x.shape[-1]
    lines = x.astype(jnp.bfloat16).reshape(near, -1, width)
    part = sum_of_blocks(lines, NEAR).astype(jnp.bfloat16)
    own = sum_of_blocks(part.reshape(far, -1, width), FAR)
    own = (own * factor).astype(jnp.bfloat16)
    part = copies(own, FAR).reshape(-1, width)
    return copies(part, NEAR).reshape(x.shape).astype(jnp.float32)


def on_device(section_input, first_pre, second_pre, out_grad, kernels, bn_scale, bn_shift):
    section_index = lax.axis_index("section")
    sections = lax.axis_size("section")
    last = section_index == sections - 1
    micros, rows_here, cols_here, width = out_grad.shape
    inputs = section_input[0]
    kernel = kernels[0]
    scales = bn_scale[0]
    shifts = bn_shift[0]
    first_norm = scales[0] * first_pre[0].astype(jnp.float32) + shifts[0]
    first_act = jnp.maximum(first_norm, 0.0).astype(jnp.bfloat16)
    second_norm = scales[1] * second_pre[0].astype(jnp.float32) + shifts[1]
    alive = second_norm + inputs.astype(jnp.float32) > 0
    one = jnp.ones((), jnp.bfloat16)
    zero = jnp.zeros((), jnp.bfloat16)
    passed = jnp.where(alive, jnp.where(last, out_grad, one), zero)
    first_on = jnp.where(first_norm > 0, one, zero)
    depth = 2 * sections
    masks = jnp.stack([passed, first_on])
    masks = with_halo(masks, COL, 3, depth)
    masks = with_halo(masks, ROW, 2, depth)
    passed, first_on = (masks[0], masks[1])
    flip_first = flip_kernel(kernel[0])
    flip_second = flip_kernel(kernel[1])

    def unit(incoming, reach):
        masked = crop(passed, depth - reach - 2)
        if incoming is not None:
            masked = masked * incoming
        masked = masked.astype(jnp.float32)
        second_grad = (scales[1] * masked).astype(jnp.bfloat16)
        act_grad = correlate(second_grad, flip_second)
        on = crop(first_on, depth - reach - 1).astype(jnp.float32)
        first_grad = (scales[0] * (act_grad * on)).astype(jnp.bfloat16)
        result = crop(masked, 2) + correlate(first_grad, flip_first)
        return (result.astype(jnp.bfloat16), first_grad, second_grad)

    received = None
    own_incoming = jnp.where(last, one, zero)
    for step in range(sections - 1):
        reach = 2 * (sections - 1 - step)
        result, _, _ = unit(received, reach)
        received = lax.ppermute(result, "section", [(sections - 1 - step, sections - 2 - step)])
        own_incoming = own_incoming + crop(received, reach - 2)
    input_grad, first_grad, second_grad = unit(own_incoming, 0)
    partial = jnp.stack(
        [
            kernel_grad(inputs, first_grad),
            kernel_grad(first_act, crop(second_grad, 1)),
        ]
    )
    pixels = micros * rows_here * lax.axis_size(ROW) * cols_here * lax.axis_size(COL)
    factor = 1.0 / jnp.sqrt(jnp.float32(pixels))
    total = total_of(partial, factor).reshape(2, 3, 3, width, width)
    return (input_grad[None], total[None])


def solution(mesh):
    split = Mesh(
        mesh.devices.reshape(mesh.shape["section"], 8, 2, 2, 4),
        ("section", "row_0", "row_1", "col_0", "col_1"),
    )
    in_specs = (
        P("section", None, ROW, COL, None),
        P("section", None, ROW, COL, None),
        P("section", None, ROW, COL, None),
        P(None, ROW, COL, None),
        P("section", None, None, None, None, None),
        P("section", None, None),
        P("section", None, None),
    )
    out_specs = (P("section", None, ROW, COL, None), P("section", None, None, None, None, None))
    return jax.shard_map(
        on_device, mesh=split, in_specs=in_specs, out_specs=out_specs, check_vma=False
    )
```

```python
import jax
import jax.numpy as jnp
from jax import lax
from jax.sharding import Mesh
from jax.sharding import PartitionSpec as P

ROW = ("row_0", "row_1")
COL = ("col_0", "col_1")
NEAR = ("row_1", "col_1")
FAR = ("row_0", "col_0")


def with_halo(cells, axis, dim, width):
    count = lax.axis_size(axis)
    size = cells.shape[dim]
    head = lax.slice_in_dim(cells, 0, width, axis=dim)
    tail = lax.slice_in_dim(cells, size - width, size, axis=dim)
    before = lax.ppermute(tail, axis, [(i, i + 1) for i in range(count - 1)])
    after = lax.ppermute(head, axis, [(i + 1, i) for i in range(count - 1)])
    return jnp.concatenate([before, cells, after], axis=dim)


def crop(field, cut):
    if cut == 0:
        return field
    return field[:, cut:-cut, cut:-cut]


def correlate(padded, kernel):
    return lax.conv_general_dilated(
        padded,
        kernel,
        (1, 1),
        "VALID",
        dimension_numbers=("NHWC", "HWIO", "NHWC"),
        preferred_element_type=jnp.float32,
    )


def flip_kernel(kernel):
    return jnp.transpose(jnp.flip(kernel, (0, 1)), (0, 1, 3, 2))


def kernel_grad(cells, padded):
    rows_here, cols_here = (cells.shape[1], cells.shape[2])
    windows = jnp.stack(
        [
            padded[:, 2 - i : 2 - i + rows_here, 2 - j : 2 - j + cols_here]
            for i in range(3)
            for j in range(3)
        ]
    )
    return jnp.einsum("mhwc,kmhwd->kcd", cells, windows, preferred_element_type=jnp.float32)


def sum_of_blocks(blocks, axes):
    parts = lax.all_to_all(blocks, axes, 0, 0, tiled=True)
    return jnp.sum(parts.astype(jnp.float32), axis=0)


def copies(block, axes):
    count = lax.axis_size(axes)
    return lax.all_to_all(jnp.broadcast_to(block[None], (count, *block.shape)), axes, 0, 0, tiled=True)


def total_of(x, factor):
    near, stack = (lax.axis_size(NEAR), lax.axis_size("row_0"))
    width = x.shape[-1]
    lines = x.astype(jnp.bfloat16).reshape(near, -1, width)
    part = sum_of_blocks(lines, NEAR).astype(jnp.bfloat16).reshape(stack, 1, -1, width)
    twice = jnp.broadcast_to(part, (stack, lax.axis_size("col_0"), *part.shape[2:]))
    own = sum_of_blocks(twice.reshape(-1, *part.shape[2:]), FAR)
    own = (own * factor).astype(jnp.bfloat16)
    part = lax.all_gather(own, "row_0", axis=0, tiled=True)
    return copies(part, NEAR).reshape(x.shape).astype(jnp.float32)


def on_device(section_input, first_pre, second_pre, out_grad, kernels, bn_scale, bn_shift):
    section_index = lax.axis_index("section")
    sections = lax.axis_size("section")
    last = section_index == sections - 1
    micros, rows_here, cols_here, width = out_grad.shape
    inputs = section_input[0]
    kernel = kernels[0]
    scales = bn_scale[0]
    shifts = bn_shift[0]
    first_norm = scales[0] * first_pre[0].astype(jnp.float32) + shifts[0]
    first_act = jnp.maximum(first_norm, 0.0).astype(jnp.bfloat16)
    second_norm = scales[1] * second_pre[0].astype(jnp.float32) + shifts[1]
    alive = second_norm + inputs.astype(jnp.float32) > 0
    one = jnp.ones((), jnp.bfloat16)
    zero = jnp.zeros((), jnp.bfloat16)
    passed = jnp.where(alive, jnp.where(last, out_grad, one), zero)
    first_on = jnp.where(first_norm > 0, one, zero)
    depth = 2 * sections
    masks = jnp.stack([passed, first_on])
    masks = with_halo(masks, COL, 3, depth)
    masks = with_halo(masks, ROW, 2, depth)
    passed, first_on = (masks[0], masks[1])
    flip_first = flip_kernel(kernel[0])
    flip_second = flip_kernel(kernel[1])

    def unit(incoming, reach):
        masked = crop(passed, depth - reach - 2)
        if incoming is not None:
            masked = masked * incoming
        masked = masked.astype(jnp.float32)
        second_grad = (scales[1] * masked).astype(jnp.bfloat16)
        act_grad = correlate(second_grad, flip_second)
        on = crop(first_on, depth - reach - 1).astype(jnp.float32)
        first_grad = (scales[0] * (act_grad * on)).astype(jnp.bfloat16)
        result = crop(masked, 2) + correlate(first_grad, flip_first)
        return (result.astype(jnp.bfloat16), first_grad, second_grad)

    received = None
    own_incoming = jnp.where(last, one, zero)
    for step in range(sections - 1):
        reach = 2 * (sections - 1 - step)
        result, _, _ = unit(received, reach)
        received = lax.ppermute(result, "section", [(sections - 1 - step, sections - 2 - step)])
        own_incoming = own_incoming + crop(received, reach - 2)
    input_grad, first_grad, second_grad = unit(own_incoming, 0)
    partial = jnp.stack(
        [
            kernel_grad(inputs, first_grad),
            kernel_grad(first_act, crop(second_grad, 1)),
        ]
    )
    pixels = micros * rows_here * lax.axis_size(ROW) * cols_here * lax.axis_size(COL)
    factor = 1.0 / jnp.sqrt(jnp.float32(pixels))
    total = total_of(partial, factor).reshape(2, 3, 3, width, width)
    return (input_grad[None], total[None])


def solution(mesh):
    split = Mesh(
        mesh.devices.reshape(mesh.shape["section"], 8, 2, 2, 4),
        ("section", "row_0", "row_1", "col_0", "col_1"),
    )
    in_specs = (
        P("section", None, ROW, COL, None),
        P("section", None, ROW, COL, None),
        P("section", None, ROW, COL, None),
        P(None, ROW, COL, None),
        P("section", None, None, None, None, None),
        P("section", None, None),
        P("section", None, None),
    )
    out_specs = (P("section", None, ROW, COL, None), P("section", None, None, None, None, None))
    return jax.shard_map(
        on_device, mesh=split, in_specs=in_specs, out_specs=out_specs, check_vma=False
    )
```

```python
import functools

import jax
import jax.numpy as jnp
from jax import lax
from jax.experimental import pallas as pl
from jax.experimental.pallas import tpu as pltpu
from jax.sharding import Mesh
from jax.sharding import PartitionSpec as P

ROW = ("row_0", "row_1")
COL = ("col_0", "col_1")
NEAR = ("row_1", "col_1")
FAR = ("row_0", "col_0")
VMEM = pl.BlockSpec(memory_space=pltpu.VMEM)
SMEM = pl.BlockSpec(memory_space=pltpu.SMEM)
PARAMS = pltpu.CompilerParams(vmem_limit_bytes=24 * 1024 * 1024)


DEPTH = 8
NARROW = 4


def prepare_kernel(last, inputs, first_pre, second_pre, out_grad, scale, shift, masks, head, tail, act):
    width = masks.shape[3]
    first_norm = scale[0] * first_pre[...].astype(jnp.float32) + shift[0]
    act[...] = jnp.maximum(first_norm, 0.0).astype(jnp.bfloat16)
    second_norm = scale[1] * second_pre[...].astype(jnp.float32) + shift[1]
    alive = second_norm + inputs[...].astype(jnp.float32) > 0
    passing = jnp.where(last[0] > 0, out_grad[...].astype(jnp.float32), 1.0)
    passed = jnp.where(alive, passing, 0.0).astype(jnp.bfloat16)
    on = jnp.where(first_norm > 0, 1.0, 0.0).astype(jnp.bfloat16)
    for kind, value in enumerate((passed, on)):
        masks[kind] = value
        head[kind] = value[:, :, :DEPTH]
        tail[kind] = value[:, :, width - DEPTH :]


def correlate(field, kernel):
    rows, cols, width = field.shape
    rows -= 2
    slabs = [field[i : i + rows].reshape(rows * cols, width) for i in range(3)]
    parts = jnp.dot(jnp.concatenate(slabs, axis=1), kernel[...], preferred_element_type=jnp.float32)
    before, here, after = [parts[:, j * width : (j + 1) * width] for j in range(3)]
    total = pltpu.roll(before, 1, 0) + here + pltpu.roll(after, rows * cols - 1, 0)
    return total.reshape(rows, cols, width)


def unit(masks, micro, incoming, first, second, scale, reach):
    top = DEPTH - reach - 2
    rows = masks.shape[2] - 2 * top
    masked = masks[0, micro, top : top + rows].astype(jnp.float32)
    if incoming is not None:
        masked = masked * incoming
    second_grad = (scale[1] * masked).astype(jnp.bfloat16)
    on = masks[1, micro, top + 1 : top + rows - 1].astype(jnp.float32)
    first_grad = (scale[0] * (correlate(second_grad, second) * on)).astype(jnp.bfloat16)
    result = masked[2 : rows - 2] + correlate(first_grad, first)
    return (result, first_grad, second_grad)


def widened(cells, frame, skip):
    rows = cells.shape[0] - 2 * skip
    value = cells[skip : skip + rows].astype(jnp.float32)
    if cells.shape[1] == frame.shape[1]:
        return value
    frame[:rows] = jnp.zeros((rows, *frame.shape[1:]), jnp.float32)
    frame[:rows, NARROW : frame.shape[1] - NARROW] = value
    return frame[:rows]


def stage_kernel(*refs, micro, reach, narrow):
    masks, first, second, scale, *received, out, frame = refs
    incoming = widened(received[0], frame, 0) if received else None
    result, _, _ = unit(masks, micro, incoming, first, second, scale, reach)
    if narrow:
        frame[: result.shape[0]] = result
        result = frame[: result.shape[0], NARROW : result.shape[1] - NARROW]
    out[...] = result.astype(jnp.bfloat16)


def filter_grad(cells, windows):
    spread = []
    for field in windows:
        rows, cols, width = field.shape
        flat = field.astype(jnp.float32).reshape(rows * cols, width)
        turned = (pltpu.roll(flat, rows * cols - 1, 0), flat, pltpu.roll(flat, 1, 0))
        spread.append(
            [
                t.reshape(rows, cols, width)[:, DEPTH : cols - DEPTH].astype(jnp.bfloat16)
                for t in turned
            ]
        )
    height = cells.shape[1]
    width = cells.shape[3]
    sides = []
    for i in range(3):
        for j in range(3):
            parts = [s[j][2 - i : 2 - i + height].reshape(-1, width) for s in spread]
            sides.append(jnp.concatenate(parts, axis=0))
    flat = cells[...].reshape(-1, width)
    side = jnp.concatenate(sides, axis=1)
    return lax.dot_general(
        flat, side, (((0,), (0,)), ((), ())), preferred_element_type=jnp.float32
    )


def last_kernel(*refs, micros, steps):
    last, masks, first, second, scale, inputs, act, *received = refs
    out, partial, frame = received[-3:]
    received = received[:-3]
    firsts, seconds = ([], [])
    for micro in range(micros):
        incoming = jnp.where(last[0] > 0, 1.0, 0.0)
        for step in range(steps):
            incoming = incoming + widened(
                received[step * micros + micro], frame.at[step], 2 * (steps - 1 - step)
            )
        result, first_grad, second_grad = unit(masks, micro, incoming, first, second, scale, 0)
        out[micro] = result[:, DEPTH : result.shape[1] - DEPTH].astype(jnp.bfloat16)
        firsts.append(first_grad)
        seconds.append(second_grad[1:-1])
    width = scale.shape[1]
    for which, (cells, windows) in enumerate(((inputs, firsts), (act, seconds))):
        total = filter_grad(cells, windows).astype(jnp.bfloat16)
        for k in range(9):
            partial[which, k] = total[:, k * width : (k + 1) * width]


def join_halo(before, cells, after, dim):
    return jnp.concatenate([before, cells, after], axis=dim)


def both_ways(head, tail, axis):
    count = lax.axis_size(axis)
    before = lax.ppermute(tail, axis, [(i, i + 1) for i in range(count - 1)])
    after = lax.ppermute(head, axis, [(i + 1, i) for i in range(count - 1)])
    return (before, after)


def matrix_of(kernel):
    width = kernel.shape[-1]
    return jnp.transpose(jnp.flip(kernel, (0, 1)), (0, 3, 1, 2)).reshape(3 * width, 3 * width)


def sum_of_blocks(blocks, axes):
    parts = lax.all_to_all(blocks, axes, 0, 0, tiled=True)
    return jnp.sum(parts.astype(jnp.float32), axis=0)


def copies(block, axes):
    count = lax.axis_size(axes)
    return lax.all_to_all(jnp.broadcast_to(block[None], (count, *block.shape)), axes, 0, 0, tiled=True)


def total_of(x, factor):
    near, stack = (lax.axis_size(NEAR), lax.axis_size("row_0"))
    width = x.shape[-1]
    part = sum_of_blocks(x.reshape(near, -1, width), NEAR).astype(jnp.bfloat16)
    part = part.reshape(stack, 1, -1, width)
    twice = jnp.broadcast_to(part, (stack, lax.axis_size("col_0"), *part.shape[2:]))
    own = sum_of_blocks(twice.reshape(-1, *part.shape[2:]), FAR)
    own = (own * factor).astype(jnp.bfloat16)
    part = copies(own, "row_0").reshape(-1, width)
    return copies(part, NEAR).reshape(x.shape).astype(jnp.float32)


def on_device(section_input, first_pre, second_pre, out_grad, kernels, bn_scale, bn_shift):
    sections = lax.axis_size("section")
    last = (lax.axis_index("section") == sections - 1).astype(jnp.int32).reshape(1)
    micros, rows_here, cols_here, width = out_grad.shape
    bf16 = jnp.bfloat16
    scale = bn_scale[0]
    two = (2, micros, rows_here)
    masks, head, tail, act = pl.pallas_call(
        prepare_kernel,
        name="prepare",
        in_specs=[SMEM] + [VMEM] * 6,
        out_specs=[VMEM] * 4,
        out_shape=[
            jax.ShapeDtypeStruct((*two, cols_here, width), bf16),
            jax.ShapeDtypeStruct((*two, DEPTH, width), bf16),
            jax.ShapeDtypeStruct((*two, DEPTH, width), bf16),
            jax.ShapeDtypeStruct(out_grad.shape, bf16),
        ],
        compiler_params=PARAMS,
    )(last, section_input[0], first_pre[0], second_pre[0], out_grad, scale, bn_shift[0])
    before, after = both_ways(head, tail, COL)
    first = matrix_of(kernels[0, 0])
    second = matrix_of(kernels[0, 1])
    masks = join_halo(before, masks, after, 3)
    before, after = both_ways(masks, masks, ROW)
    masks = join_halo(before, masks, after, 2)
    high, wide = masks.shape[2:4]
    frame = pltpu.VMEM((high, wide, width), jnp.float32)

    received = [[]]
    for step in range(sections - 1):
        reach = 2 * (sections - 1 - step)
        narrow = NARROW if step else 0
        sent = []
        for micro in range(micros):
            taken = [received[-1][micro]] if step else []
            result = pl.pallas_call(
                functools.partial(stage_kernel, micro=micro, reach=reach, narrow=bool(step)),
                name=f"stage_{step}_{micro}",
                in_specs=[VMEM] * (4 + len(taken)),
                out_specs=VMEM,
                out_shape=jax.ShapeDtypeStruct(
                    (rows_here + 2 * reach, wide - 2 * narrow, width), bf16
                ),
                scratch_shapes=[frame],
                compiler_params=PARAMS,
            )(masks, first, second, scale, *taken)
            pair = [(sections - 1 - step, sections - 2 - step)]
            sent.append(lax.ppermute(result, "section", pair))
        received.append(sent)
    taken = sum(received, [])
    input_grad, partial = pl.pallas_call(
        functools.partial(last_kernel, micros=micros, steps=sections - 1),
        name="last",
        in_specs=[SMEM] + [VMEM] * (6 + len(taken)),
        out_specs=[VMEM] * 2,
        out_shape=[
            jax.ShapeDtypeStruct(out_grad.shape, bf16),
            jax.ShapeDtypeStruct((2, 9, width, width), bf16),
        ],
        scratch_shapes=[pltpu.VMEM((sections - 1, high, wide, width), jnp.float32)],
        compiler_params=PARAMS,
    )(last, masks, first, second, scale, section_input[0], act, *taken)
    pixels = micros * rows_here * lax.axis_size(ROW) * cols_here * lax.axis_size(COL)
    factor = 1.0 / jnp.sqrt(jnp.float32(pixels))
    total = total_of(partial, factor).reshape(2, 3, 3, width, width)
    return (input_grad[None], total[None])


def solution(mesh):
    split = Mesh(
        mesh.devices.reshape(mesh.shape["section"], 8, 2, 2, 4),
        ("section", "row_0", "row_1", "col_0", "col_1"),
    )
    in_specs = (
        P("section", None, ROW, COL, None),
        P("section", None, ROW, COL, None),
        P("section", None, ROW, COL, None),
        P(None, ROW, COL, None),
        P("section", None, None, None, None, None),
        P("section", None, None),
        P("section", None, None),
    )
    out_specs = (P("section", None, ROW, COL, None), P("section", None, None, None, None, None))
    return jax.shard_map(
        on_device, mesh=split, in_specs=in_specs, out_specs=out_specs, check_vma=False
    )
```

```python
import functools

import jax
import jax.numpy as jnp
from jax import lax
from jax.experimental import pallas as pl
from jax.experimental.pallas import tpu as pltpu
from jax.sharding import Mesh
from jax.sharding import PartitionSpec as P

ROW = ("row_0", "row_1")
COL = ("col_0", "col_1")
NEAR = ("row_1", "col_1")
FAR = ("row_0", "col_0")
VMEM = pl.BlockSpec(memory_space=pltpu.VMEM)
SMEM = pl.BlockSpec(memory_space=pltpu.SMEM)
PARAMS = pltpu.CompilerParams(vmem_limit_bytes=24 * 1024 * 1024)


DEPTH = 8
NARROW = 4


def prepare_kernel(flags, *refs):
    sources = refs[:6]
    masks, inward, outward, act, fields, norms, done = refs[6:]
    targets = [fields.at[k] for k in range(4)] + [norms.at[k] for k in range(2)]
    moves = [
        pltpu.make_async_copy(source, target, done.at[k])
        for k, (source, target) in enumerate(zip(sources, targets))
    ]
    for move in moves:
        move.start()
    for move in moves:
        move.wait()
    inputs, first_pre, second_pre, out_grad = [fields[k].astype(jnp.float32) for k in range(4)]
    scale, shift = (norms[0], norms[1])
    width = masks.shape[3]
    first_norm = scale[0] * first_pre + shift[0]
    act[...] = jnp.maximum(first_norm, 0.0).astype(jnp.bfloat16)
    alive = scale[1] * second_pre + shift[1] + inputs > 0
    passing = jnp.where(flags[0] > 0, out_grad, 1.0)
    passed = jnp.where(alive, passing, 0.0)
    on = jnp.where(first_norm > 0, 1.0, 0.0)
    for kind, value in enumerate((passed, on)):
        masks[kind] = value.astype(jnp.bfloat16)
        head = value[:, :, :DEPTH]
        tail = value[:, :, width - DEPTH :]
        inward[kind] = jnp.where(flags[1] > 0, tail, head).astype(jnp.bfloat16)
        outward[kind] = jnp.where(flags[1] > 0, head, tail).astype(jnp.bfloat16)


def correlate(field, kernel):
    rows, cols, width = field.shape
    rows -= 2
    slabs = [field[i : i + rows].reshape(rows * cols, width) for i in range(3)]
    parts = jnp.dot(jnp.concatenate(slabs, axis=1), kernel[...], preferred_element_type=jnp.float32)
    before, here, after = [parts[:, j * width : (j + 1) * width] for j in range(3)]
    total = pltpu.roll(before, 1, 0) + here + pltpu.roll(after, rows * cols - 1, 0)
    return total.reshape(rows, cols, width)


def unit(masks, micro, incoming, first, second, scale, reach):
    top = DEPTH - reach - 2
    rows = masks.shape[2] - 2 * top
    masked = masks[0, micro, top : top + rows].astype(jnp.float32)
    if incoming is not None:
        masked = masked * incoming
    second_grad = (scale[1] * masked).astype(jnp.bfloat16)
    on = masks[1, micro, top + 1 : top + rows - 1].astype(jnp.float32)
    first_grad = (scale[0] * (correlate(second_grad, second) * on)).astype(jnp.bfloat16)
    result = masked[2 : rows - 2] + correlate(first_grad, first)
    return (result, first_grad, second_grad)


def widened(cells, frame, skip):
    rows = cells.shape[0] - 2 * skip
    value = cells[skip : skip + rows].astype(jnp.float32)
    if cells.shape[1] == frame.shape[1]:
        return value
    frame[:rows] = jnp.zeros((rows, *frame.shape[1:]), jnp.float32)
    frame[:rows, NARROW : frame.shape[1] - NARROW] = value
    return frame[:rows]


def stage_kernel(*refs, micro, reach, narrow):
    masks, first, second, scale, *received, out, frame = refs
    incoming = widened(received[0], frame, 0) if received else None
    result, _, _ = unit(masks, micro, incoming, first, second, scale, reach)
    if narrow:
        frame[: result.shape[0]] = result
        result = frame[: result.shape[0], NARROW : result.shape[1] - NARROW]
    out[...] = result.astype(jnp.bfloat16)


def filter_grad(cells, windows):
    spread = []
    for field in windows:
        rows, cols, width = field.shape
        flat = field.astype(jnp.float32).reshape(rows * cols, width)
        turned = (pltpu.roll(flat, rows * cols - 1, 0), flat, pltpu.roll(flat, 1, 0))
        spread.append(
            [
                t.reshape(rows, cols, width)[:, DEPTH : cols - DEPTH].astype(jnp.bfloat16)
                for t in turned
            ]
        )
    height = cells.shape[1]
    width = cells.shape[3]
    sides = []
    for i in range(3):
        for j in range(3):
            parts = [s[j][2 - i : 2 - i + height].reshape(-1, width) for s in spread]
            sides.append(jnp.concatenate(parts, axis=0))
    flat = cells[...].reshape(-1, width)
    side = jnp.concatenate(sides, axis=1)
    return lax.dot_general(
        flat, side, (((0,), (0,)), ((), ())), preferred_element_type=jnp.float32
    )


def settle(last, masks, micro, received, first, second, scale, frame):
    incoming = jnp.where(last[0] > 0, 1.0, 0.0)
    steps = len(received)
    for step, cells in enumerate(received):
        incoming = incoming + widened(cells, frame.at[step], 2 * (steps - 1 - step))
    result, first_grad, second_grad = unit(masks, micro, incoming, first, second, scale, 0)
    tile = result[:, DEPTH : result.shape[1] - DEPTH].astype(jnp.bfloat16)
    return (tile, first_grad, second_grad[1:-1])


def early_kernel(*refs, micro):
    last, masks, first, second, scale, *received, tile, first_grad, second_grad, frame = refs
    values = settle(last, masks, micro, received, first, second, scale, frame)
    for ref, value in zip((tile, first_grad, second_grad), values):
        ref[...] = value


def last_kernel(*refs, micros, early):
    last, masks, first, second, scale, inputs, act, *rest = refs
    out, partial, frame = rest[-3:]
    ready = rest[: 3 * early]
    received = rest[3 * early : -3]
    units = [[ref[...] for ref in ready[3 * m : 3 * m + 3]] for m in range(early)]
    units.append(settle(last, masks, micros - 1, received, first, second, scale, frame))
    for micro, (tile, _, _) in enumerate(units):
        out[micro] = tile
    width = scale.shape[1]
    for which, cells in enumerate((inputs, act)):
        total = filter_grad(cells, [u[1 + which] for u in units]).astype(jnp.bfloat16)
        for k in range(9):
            partial[which, k] = total[:, k * width : (k + 1) * width]


def swaps(inward, outward, axis):
    count = lax.axis_size(axis)
    crossing = [(i, i + 1) for i in range(1, count - 1, 2)]
    apart = lax.ppermute(outward, axis, crossing + [(j, i) for i, j in crossing])
    close = lax.ppermute(inward, axis, [(i, i ^ 1) for i in range(count)])
    even = (lax.axis_index(axis) & 1) == 0
    return (jnp.where(even, apart, close), jnp.where(even, close, apart))


def matrix_of(kernel):
    width = kernel.shape[-1]
    return jnp.transpose(jnp.flip(kernel, (0, 1)), (0, 3, 1, 2)).reshape(3 * width, 3 * width)


def sum_of_blocks(blocks, axes):
    parts = lax.all_to_all(blocks, axes, 0, 0, tiled=True)
    return jnp.sum(parts.astype(jnp.float32), axis=0)


def copies(block, axes):
    count = lax.axis_size(axes)
    return lax.all_to_all(jnp.broadcast_to(block[None], (count, *block.shape)), axes, 0, 0, tiled=True)


def total_of(x, factor):
    near, stack = (lax.axis_size(NEAR), lax.axis_size("row_0"))
    width = x.shape[-1]
    part = sum_of_blocks(x.reshape(near, -1, width), NEAR).astype(jnp.bfloat16)
    part = part.reshape(stack, 1, -1, width)
    twice = jnp.broadcast_to(part, (stack, lax.axis_size("col_0"), *part.shape[2:]))
    own = sum_of_blocks(twice.reshape(-1, *part.shape[2:]), FAR)
    own = (own * factor).astype(jnp.bfloat16)
    part = copies(own, "row_0").reshape(-1, width)
    return copies(part, NEAR).reshape(x.shape).astype(jnp.float32)


def on_device(section_input, first_pre, second_pre, out_grad, kernels, bn_scale, bn_shift):
    sections = lax.axis_size("section")
    last = (lax.axis_index("section") == sections - 1).astype(jnp.int32).reshape(1)
    even = ((lax.axis_index(COL) & 1) == 0).astype(jnp.int32).reshape(1)
    micros, rows_here, cols_here, width = out_grad.shape
    bf16 = jnp.bfloat16
    scale = bn_scale[0]
    two = (2, micros, rows_here)
    masks, inward, outward, act = pl.pallas_call(
        prepare_kernel,
        name="prepare",
        in_specs=[SMEM] + [pl.BlockSpec(memory_space=pltpu.MemorySpace.HBM)] * 6,
        out_specs=[VMEM] * 4,
        out_shape=[
            jax.ShapeDtypeStruct((*two, cols_here, width), bf16),
            jax.ShapeDtypeStruct((*two, DEPTH, width), bf16),
            jax.ShapeDtypeStruct((*two, DEPTH, width), bf16),
            jax.ShapeDtypeStruct(out_grad.shape, bf16),
        ],
        scratch_shapes=[
            pltpu.VMEM((4, *out_grad.shape), bf16),
            pltpu.VMEM((2, *scale.shape), jnp.float32),
            pltpu.SemaphoreType.DMA((6,)),
        ],
        compiler_params=PARAMS,
    )(
        jnp.concatenate([last, even]),
        *[
            pltpu.with_memory_space_constraint(x, pltpu.MemorySpace.HBM)
            for x in (section_input[0], first_pre[0], second_pre[0], out_grad, scale, bn_shift[0])
        ],
    )
    left, right = swaps(inward, outward, COL)
    above, below = swaps(masks, masks, ROW)
    sides = jnp.concatenate([left, right], axis=3)
    above_sides, below_sides = swaps(sides, sides, ROW)
    first = matrix_of(kernels[0, 0])
    second = matrix_of(kernels[0, 1])
    bands = [
        jnp.concatenate([side[:, :, :, :DEPTH], middle, side[:, :, :, DEPTH:]], axis=3)
        for side, middle in ((above_sides, above), (sides, masks), (below_sides, below))
    ]
    masks = jnp.concatenate(bands, axis=2)
    high, wide = masks.shape[2:4]
    frame = pltpu.VMEM((high, wide, width), jnp.float32)

    received = [[]]
    for step in range(sections - 1):
        reach = 2 * (sections - 1 - step)
        narrow = NARROW if step else 0
        sent = []
        for micro in range(micros):
            taken = [received[-1][micro]] if step else []
            result = pl.pallas_call(
                functools.partial(stage_kernel, micro=micro, reach=reach, narrow=bool(step)),
                name=f"stage_{step}_{micro}",
                in_specs=[VMEM] * (4 + len(taken)),
                out_specs=VMEM,
                out_shape=jax.ShapeDtypeStruct(
                    (rows_here + 2 * reach, wide - 2 * narrow, width), bf16
                ),
                scratch_shapes=[frame],
                compiler_params=PARAMS,
            )(masks, first, second, scale, *taken)
            pair = [(sections - 1 - step, sections - 2 - step)]
            sent.append(lax.ppermute(result, "section", pair))
        received.append(sent)
    frames = pltpu.VMEM((sections - 1, high, wide, width), jnp.float32)
    common = (last, masks, first, second, scale)
    arrived = [[step[micro] for step in received[1:]] for micro in range(micros)]
    ready = []
    for micro in range(micros - 1):
        field = jax.ShapeDtypeStruct((rows_here + 2, wide, width), bf16)
        ready += pl.pallas_call(
            functools.partial(early_kernel, micro=micro),
            name=f"early_{micro}",
            in_specs=[SMEM] + [VMEM] * (4 + len(arrived[micro])),
            out_specs=[VMEM] * 3,
            out_shape=[jax.ShapeDtypeStruct(out_grad.shape[1:], bf16), field, field],
            scratch_shapes=[frames],
            compiler_params=PARAMS,
        )(*common, *arrived[micro])
    taken = ready + arrived[-1]
    input_grad, partial = pl.pallas_call(
        functools.partial(last_kernel, micros=micros, early=micros - 1),
        name="last",
        in_specs=[SMEM] + [VMEM] * (6 + len(taken)),
        out_specs=[VMEM] * 2,
        out_shape=[
            jax.ShapeDtypeStruct(out_grad.shape, bf16),
            jax.ShapeDtypeStruct((2, 9, width, width), bf16),
        ],
        scratch_shapes=[frames],
        compiler_params=PARAMS,
    )(*common, section_input[0], act, *taken)
    pixels = micros * rows_here * lax.axis_size(ROW) * cols_here * lax.axis_size(COL)
    factor = 1.0 / jnp.sqrt(jnp.float32(pixels))
    total = total_of(partial, factor).reshape(2, 3, 3, width, width)
    return (input_grad[None], total[None])


def solution(mesh):
    split = Mesh(
        mesh.devices.reshape(mesh.shape["section"], 8, 2, 2, 4),
        ("section", "row_0", "row_1", "col_0", "col_1"),
    )
    in_specs = (
        P("section", None, ROW, COL, None),
        P("section", None, ROW, COL, None),
        P("section", None, ROW, COL, None),
        P(None, ROW, COL, None),
        P("section", None, None, None, None, None),
        P("section", None, None),
        P("section", None, None),
    )
    out_specs = (P("section", None, ROW, COL, None), P("section", None, None, None, None, None))
    return jax.shard_map(
        on_device, mesh=split, in_specs=in_specs, out_specs=out_specs, check_vma=False
    )
```

```python
import functools

import jax
import jax.numpy as jnp
from jax import lax
from jax.experimental import pallas as pl
from jax.experimental.pallas import tpu as pltpu
from jax.sharding import Mesh
from jax.sharding import PartitionSpec as P

ROW = ("row_0", "row_1")
COL = ("col_0", "col_1")
NEAR = ("row_1", "col_1")
FAR = ("row_0", "col_0")
VMEM = pl.BlockSpec(memory_space=pltpu.VMEM)
SMEM = pl.BlockSpec(memory_space=pltpu.SMEM)
PARAMS = pltpu.CompilerParams(vmem_limit_bytes=24 * 1024 * 1024)


DEPTH = 8
NARROW = 4


def prepare_kernel(flags, *refs):
    sources = refs[:6]
    masks, inward, outward, act, kept, fields, norms, done = refs[6:]
    targets = [fields.at[k] for k in range(4)] + [norms.at[k] for k in range(2)]
    moves = [
        pltpu.make_async_copy(source, target, done.at[k])
        for k, (source, target) in enumerate(zip(sources, targets))
    ]
    for move in moves:
        move.start()
    for move in moves:
        move.wait()
    inputs, first_pre, second_pre, out_grad = [fields[k].astype(jnp.float32) for k in range(4)]
    scale, shift = (norms[0], norms[1])
    kept[...] = scale
    width = masks.shape[3]
    first_norm = scale[0] * first_pre + shift[0]
    act[...] = jnp.maximum(first_norm, 0.0).astype(jnp.bfloat16)
    alive = scale[1] * second_pre + shift[1] + inputs > 0
    passing = jnp.where(flags[0] > 0, out_grad, 1.0)
    passed = jnp.where(alive, passing, 0.0)
    on = jnp.where(first_norm > 0, 1.0, 0.0)
    for kind, value in enumerate((passed, on)):
        masks[kind] = value.astype(jnp.bfloat16)
        head = value[:, :, :DEPTH]
        tail = value[:, :, width - DEPTH :]
        inward[kind] = jnp.where(flags[1] > 0, tail, head).astype(jnp.bfloat16)
        outward[kind] = jnp.where(flags[1] > 0, head, tail).astype(jnp.bfloat16)


def correlate(field, kernel):
    rows, cols, width = field.shape
    rows -= 2
    slabs = [field[i : i + rows].reshape(rows * cols, width) for i in range(3)]
    parts = jnp.dot(jnp.concatenate(slabs, axis=1), kernel[...], preferred_element_type=jnp.float32)
    before, here, after = [parts[:, j * width : (j + 1) * width] for j in range(3)]
    total = pltpu.roll(before, 1, 0) + here + pltpu.roll(after, rows * cols - 1, 0)
    return total.reshape(rows, cols, width)


def unit(masks, micro, incoming, first, second, scale, reach):
    top = DEPTH - reach - 2
    rows = masks.shape[2] - 2 * top
    masked = masks[0, micro, top : top + rows].astype(jnp.float32)
    if incoming is not None:
        masked = masked * incoming
    second_grad = (scale[1] * masked).astype(jnp.bfloat16)
    on = masks[1, micro, top + 1 : top + rows - 1].astype(jnp.float32)
    first_grad = (scale[0] * (correlate(second_grad, second) * on)).astype(jnp.bfloat16)
    result = masked[2 : rows - 2] + correlate(first_grad, first)
    return (result, first_grad, second_grad)


def widened(cells, frame, skip):
    rows = cells.shape[0] - 2 * skip
    value = cells[skip : skip + rows].astype(jnp.float32)
    if cells.shape[1] == frame.shape[1]:
        return value
    frame[:rows] = jnp.zeros((rows, *frame.shape[1:]), jnp.float32)
    frame[:rows, NARROW : frame.shape[1] - NARROW] = value
    return frame[:rows]


def stage_kernel(*refs, micro, reach, narrow):
    masks, first, second, scale, *received, out, frame = refs
    incoming = widened(received[0], frame, 0) if received else None
    result, _, _ = unit(masks, micro, incoming, first, second, scale, reach)
    if narrow:
        frame[: result.shape[0]] = result
        result = frame[: result.shape[0], NARROW : result.shape[1] - NARROW]
    out[...] = result.astype(jnp.bfloat16)


def filter_grad(cells, windows):
    spread = []
    for field in windows:
        rows, cols, width = field.shape
        flat = field.astype(jnp.float32).reshape(rows * cols, width)
        turned = (pltpu.roll(flat, rows * cols - 1, 0), flat, pltpu.roll(flat, 1, 0))
        spread.append(
            [
                t.reshape(rows, cols, width)[:, DEPTH : cols - DEPTH].astype(jnp.bfloat16)
                for t in turned
            ]
        )
    height = cells.shape[1]
    width = cells.shape[3]
    sides = []
    for i in range(3):
        for j in range(3):
            parts = [s[j][2 - i : 2 - i + height].reshape(-1, width) for s in spread]
            sides.append(jnp.concatenate(parts, axis=0))
    flat = cells[...].reshape(-1, width)
    side = jnp.concatenate(sides, axis=1)
    return lax.dot_general(
        flat, side, (((0,), (0,)), ((), ())), preferred_element_type=jnp.float32
    )


def settle(last, masks, micro, received, first, second, scale, frame):
    incoming = jnp.where(last[0] > 0, 1.0, 0.0)
    steps = len(received)
    for step, cells in enumerate(received):
        incoming = incoming + widened(cells, frame.at[step], 2 * (steps - 1 - step))
    result, first_grad, second_grad = unit(masks, micro, incoming, first, second, scale, 0)
    tile = result[:, DEPTH : result.shape[1] - DEPTH].astype(jnp.bfloat16)
    return (tile, first_grad, second_grad[1:-1])


def early_kernel(*refs, micro):
    last, masks, first, second, scale, *received, tile, first_grad, second_grad, frame = refs
    values = settle(last, masks, micro, received, first, second, scale, frame)
    for ref, value in zip((tile, first_grad, second_grad), values):
        ref[...] = value


def last_kernel(*refs, micros, early):
    last, masks, first, second, scale, inputs, act, *rest = refs
    out, partial, frame = rest[-3:]
    ready = rest[: 3 * early]
    received = rest[3 * early : -3]
    units = [[ref[...] for ref in ready[3 * m : 3 * m + 3]] for m in range(early)]
    units.append(settle(last, masks, micros - 1, received, first, second, scale, frame))
    for micro, (tile, _, _) in enumerate(units):
        out[micro] = tile
    width = scale.shape[1]
    for which, cells in enumerate((inputs, act)):
        total = filter_grad(cells, [u[1 + which] for u in units]).astype(jnp.bfloat16)
        for k in range(9):
            partial[which, k] = total[:, k * width : (k + 1) * width]


def swaps(inward, outward, axis):
    count = lax.axis_size(axis)
    crossing = [(i, i + 1) for i in range(1, count - 1, 2)]
    apart = lax.ppermute(outward, axis, crossing + [(j, i) for i, j in crossing])
    close = lax.ppermute(inward, axis, [(i, i ^ 1) for i in range(count)])
    even = (lax.axis_index(axis) & 1) == 0
    return (jnp.where(even, apart, close), jnp.where(even, close, apart))


def matrix_of(kernel):
    width = kernel.shape[-1]
    return jnp.transpose(jnp.flip(kernel, (0, 1)), (0, 3, 1, 2)).reshape(3 * width, 3 * width)


def sum_of_blocks(blocks, axes):
    parts = lax.all_to_all(blocks, axes, 0, 0, tiled=True)
    return jnp.sum(parts.astype(jnp.float32), axis=0)


def copies(block, axes):
    count = lax.axis_size(axes)
    return lax.all_to_all(jnp.broadcast_to(block[None], (count, *block.shape)), axes, 0, 0, tiled=True)


def total_of(x, factor):
    near, stack = (lax.axis_size(NEAR), lax.axis_size("row_0"))
    width = x.shape[-1]
    part = sum_of_blocks(x.reshape(near, -1, width), NEAR).astype(jnp.bfloat16)
    part = part.reshape(stack, 1, -1, width)
    twice = jnp.broadcast_to(part, (stack, lax.axis_size("col_0"), *part.shape[2:]))
    own = sum_of_blocks(twice.reshape(-1, *part.shape[2:]), FAR)
    own = (own * factor).astype(jnp.bfloat16)
    part = copies(own, "row_0").reshape(-1, width)
    return copies(part, NEAR).reshape(x.shape).astype(jnp.float32)


def section_backward(section_input, first_pre, second_pre, out_grad, kernels, bn_scale, bn_shift):
    sections = lax.axis_size("section")
    last = (lax.axis_index("section") == sections - 1).astype(jnp.int32).reshape(1)
    even = ((lax.axis_index(COL) & 1) == 0).astype(jnp.int32).reshape(1)
    micros, rows_here, cols_here, width = out_grad.shape
    bf16 = jnp.bfloat16
    scale = bn_scale[0]
    two = (2, micros, rows_here)
    masks, inward, outward, act, scale = pl.pallas_call(
        prepare_kernel,
        name="prepare",
        in_specs=[SMEM] + [pl.BlockSpec(memory_space=pltpu.MemorySpace.HBM)] * 6,
        out_specs=[VMEM] * 5,
        out_shape=[
            jax.ShapeDtypeStruct((*two, cols_here, width), bf16),
            jax.ShapeDtypeStruct((*two, DEPTH, width), bf16),
            jax.ShapeDtypeStruct((*two, DEPTH, width), bf16),
            jax.ShapeDtypeStruct(out_grad.shape, bf16),
            jax.ShapeDtypeStruct(scale.shape, jnp.float32),
        ],
        scratch_shapes=[
            pltpu.VMEM((4, *out_grad.shape), bf16),
            pltpu.VMEM((2, *scale.shape), jnp.float32),
            pltpu.SemaphoreType.DMA((6,)),
        ],
        compiler_params=PARAMS,
    )(
        jnp.concatenate([last, even]),
        *[
            pltpu.with_memory_space_constraint(x, pltpu.MemorySpace.HBM)
            for x in (section_input[0], first_pre[0], second_pre[0], out_grad, scale, bn_shift[0])
        ],
    )
    left, right = swaps(inward, outward, COL)
    above, below = swaps(masks, masks, ROW)
    sides = jnp.concatenate([left, right], axis=3)
    sides, kernels = lax.optimization_barrier((sides, kernels))
    above_sides, below_sides = swaps(sides, sides, ROW)
    first = matrix_of(kernels[0, 0])
    second = matrix_of(kernels[0, 1])
    bands = [
        jnp.concatenate([side[:, :, :, :DEPTH], middle, side[:, :, :, DEPTH:]], axis=3)
        for side, middle in ((above_sides, above), (sides, masks), (below_sides, below))
    ]
    masks = jnp.concatenate(bands, axis=2)
    high, wide = masks.shape[2:4]
    frame = pltpu.VMEM((high, wide, width), jnp.float32)

    received = [[]]
    for step in range(sections - 1):
        reach = 2 * (sections - 1 - step)
        narrow = NARROW if step else 0
        sent = []
        for micro in range(micros):
            taken = [received[-1][micro]] if step else []
            result = pl.pallas_call(
                functools.partial(stage_kernel, micro=micro, reach=reach, narrow=bool(step)),
                in_specs=[VMEM] * (4 + len(taken)),
                out_specs=VMEM,
                out_shape=jax.ShapeDtypeStruct(
                    (rows_here + 2 * reach, wide - 2 * narrow, width), bf16
                ),
                scratch_shapes=[frame],
                compiler_params=PARAMS,
            )(masks, first, second, scale, *taken)
            pair = [(sections - 1 - step, sections - 2 - step)]
            sent.append(lax.ppermute(result, "section", pair))
        received.append(sent)
    frames = pltpu.VMEM((sections - 1, high, wide, width), jnp.float32)
    common = (last, masks, first, second, scale)
    arrived = [[step[micro] for step in received[1:]] for micro in range(micros)]
    ready = []
    for micro in range(micros - 1):
        field = jax.ShapeDtypeStruct((rows_here + 2, wide, width), bf16)
        ready += pl.pallas_call(
            functools.partial(early_kernel, micro=micro),
            in_specs=[SMEM] + [VMEM] * (4 + len(arrived[micro])),
            out_specs=[VMEM] * 3,
            out_shape=[jax.ShapeDtypeStruct(out_grad.shape[1:], bf16), field, field],
            scratch_shapes=[frames],
            compiler_params=PARAMS,
        )(*common, *arrived[micro])
    taken = ready + arrived[-1]
    input_grad, partial = pl.pallas_call(
        functools.partial(last_kernel, micros=micros, early=micros - 1),
        name="last",
        in_specs=[SMEM] + [VMEM] * (6 + len(taken)),
        out_specs=[VMEM] * 2,
        out_shape=[
            jax.ShapeDtypeStruct(out_grad.shape, bf16),
            jax.ShapeDtypeStruct((2, 9, width, width), bf16),
        ],
        scratch_shapes=[frames],
        compiler_params=PARAMS,
    )(*common, section_input[0], act, *taken)
    pixels = micros * rows_here * lax.axis_size(ROW) * cols_here * lax.axis_size(COL)
    factor = 1.0 / jnp.sqrt(jnp.float32(pixels))
    total = total_of(partial, factor).reshape(2, 3, 3, width, width)
    return (input_grad[None], total[None])


def solution(mesh):
    split = Mesh(
        mesh.devices.reshape(mesh.shape["section"], 8, 2, 2, 4),
        ("section", "row_0", "row_1", "col_0", "col_1"),
    )
    in_specs = (
        P("section", None, ROW, COL, None),
        P("section", None, ROW, COL, None),
        P("section", None, ROW, COL, None),
        P(None, ROW, COL, None),
        P("section", None, None, None, None, None),
        P("section", None, None),
        P("section", None, None),
    )
    out_specs = (P("section", None, ROW, COL, None), P("section", None, None, None, None, None))
    return jax.shard_map(
        section_backward, mesh=split, in_specs=in_specs, out_specs=out_specs, check_vma=False
    )
```

```python
import functools

import jax
import jax.numpy as jnp
from jax import lax
from jax.experimental import pallas as pl
from jax.experimental.pallas import tpu as pltpu
from jax.sharding import Mesh
from jax.sharding import PartitionSpec as P

ROW = ("row_0", "row_1")
COL = ("col_0", "col_1")
NEAR = ("row_1", "col_1")
FAR = ("row_0", "col_0")
VMEM = pl.BlockSpec(memory_space=pltpu.VMEM)
SMEM = pl.BlockSpec(memory_space=pltpu.SMEM)
PARAMS = pltpu.CompilerParams(vmem_limit_bytes=24 * 1024 * 1024)


DEPTH = 8
NARROW = 4


def prepare_kernel(flags, *refs):
    sources = refs[:6]
    masks, inward, outward, act, kept, fields, norms, done = refs[6:]
    targets = [fields.at[k] for k in range(4)] + [norms.at[k] for k in range(2)]
    moves = [
        pltpu.make_async_copy(source, target, done.at[k])
        for k, (source, target) in enumerate(zip(sources, targets))
    ]
    for move in moves:
        move.start()
    for move in moves:
        move.wait()
    inputs, first_pre, second_pre, out_grad = [fields[k].astype(jnp.float32) for k in range(4)]
    scale, shift = (norms[0], norms[1])
    kept[...] = scale
    width = masks.shape[3]
    first_norm = scale[0] * first_pre + shift[0]
    act[...] = jnp.maximum(first_norm, 0.0).astype(jnp.bfloat16)
    alive = scale[1] * second_pre + shift[1] + inputs > 0
    passing = jnp.where(flags[0] > 0, out_grad, 1.0)
    passed = jnp.where(alive, passing, 0.0)
    on = jnp.where(first_norm > 0, 1.0, 0.0)
    for kind, value in enumerate((passed, on)):
        masks[kind] = value.astype(jnp.bfloat16)
        head = value[:, :, :DEPTH]
        tail = value[:, :, width - DEPTH :]
        inward[kind] = jnp.where(flags[1] > 0, tail, head).astype(jnp.bfloat16)
        outward[kind] = jnp.where(flags[1] > 0, head, tail).astype(jnp.bfloat16)


def correlate(field, kernel):
    rows, cols, width = field.shape
    rows -= 2
    slabs = [field[i : i + rows].reshape(rows * cols, width) for i in range(3)]
    parts = jnp.dot(jnp.concatenate(slabs, axis=1), kernel[...], preferred_element_type=jnp.float32)
    before, here, after = [parts[:, j * width : (j + 1) * width] for j in range(3)]
    total = pltpu.roll(before, 1, 0) + here + pltpu.roll(after, rows * cols - 1, 0)
    return total.reshape(rows, cols, width)


def unit(masks, micro, incoming, first, second, scale, reach):
    top = DEPTH - reach - 2
    rows = masks.shape[2] - 2 * top
    masked = masks[0, micro, top : top + rows].astype(jnp.float32)
    if incoming is not None:
        masked = masked * incoming
    second_grad = (scale[1] * masked).astype(jnp.bfloat16)
    on = masks[1, micro, top + 1 : top + rows - 1].astype(jnp.float32)
    first_grad = (scale[0] * (correlate(second_grad, second) * on)).astype(jnp.bfloat16)
    result = masked[2 : rows - 2] + correlate(first_grad, first)
    return (result, first_grad, second_grad)


def widened(cells, frame, skip):
    rows = cells.shape[0] - 2 * skip
    value = cells[skip : skip + rows].astype(jnp.float32)
    if cells.shape[1] == frame.shape[1]:
        return value
    frame[:rows] = jnp.zeros((rows, *frame.shape[1:]), jnp.float32)
    frame[:rows, NARROW : frame.shape[1] - NARROW] = value
    return frame[:rows]


def stage_kernel(*refs, micro, reach, narrow):
    masks, first, second, scale, *received, out, frame = refs
    incoming = widened(received[0], frame, 0) if received else None
    result, _, _ = unit(masks, micro, incoming, first, second, scale, reach)
    if narrow:
        frame[: result.shape[0]] = result
        result = frame[: result.shape[0], NARROW : result.shape[1] - NARROW]
    out[...] = result.astype(jnp.bfloat16)


def filter_grad(cells, windows):
    spread = []
    for field in windows:
        rows, cols, width = field.shape
        flat = field.astype(jnp.float32).reshape(rows * cols, width)
        turned = (pltpu.roll(flat, rows * cols - 1, 0), flat, pltpu.roll(flat, 1, 0))
        spread.append(
            [
                t.reshape(rows, cols, width)[:, DEPTH : cols - DEPTH].astype(jnp.bfloat16)
                for t in turned
            ]
        )
    height = cells.shape[1]
    width = cells.shape[3]
    sides = []
    for i in range(3):
        for j in range(3):
            parts = [s[j][2 - i : 2 - i + height].reshape(-1, width) for s in spread]
            sides.append(jnp.concatenate(parts, axis=0))
    flat = cells[...].reshape(-1, width)
    side = jnp.concatenate(sides, axis=1)
    return lax.dot_general(
        flat, side, (((0,), (0,)), ((), ())), preferred_element_type=jnp.float32
    )


def settle(last, masks, micro, received, first, second, scale, frame):
    incoming = jnp.where(last[0] > 0, 1.0, 0.0)
    steps = len(received)
    for step, cells in enumerate(received):
        incoming = incoming + widened(cells, frame.at[step], 2 * (steps - 1 - step))
    result, first_grad, second_grad = unit(masks, micro, incoming, first, second, scale, 0)
    tile = result[:, DEPTH : result.shape[1] - DEPTH].astype(jnp.bfloat16)
    return (tile, first_grad, second_grad[1:-1])


def early_kernel(*refs, micro):
    last, masks, first, second, scale, *received, tile, first_grad, second_grad, frame = refs
    values = settle(last, masks, micro, received, first, second, scale, frame)
    for ref, value in zip((tile, first_grad, second_grad), values):
        ref[...] = value


def last_kernel(*refs, micros, early):
    last, masks, first, second, scale, inputs, act, *rest = refs
    out, partial, frame = rest[-3:]
    ready = rest[: 3 * early]
    received = rest[3 * early : -3]
    units = [[ref[...] for ref in ready[3 * m : 3 * m + 3]] for m in range(early)]
    units.append(settle(last, masks, micros - 1, received, first, second, scale, frame))
    for micro, (tile, _, _) in enumerate(units):
        out[micro] = tile
    width = scale.shape[1]
    for which, cells in enumerate((inputs, act)):
        total = filter_grad(cells, [u[1 + which] for u in units]).astype(jnp.bfloat16)
        for k in range(9):
            partial[which, k] = total[:, k * width : (k + 1) * width]


def swaps(inward, outward, axis):
    count = lax.axis_size(axis)
    crossing = [(i, i + 1) for i in range(1, count - 1, 2)]
    apart = lax.ppermute(outward, axis, crossing + [(j, i) for i, j in crossing])
    close = lax.ppermute(inward, axis, [(i, i ^ 1) for i in range(count)])
    even = (lax.axis_index(axis) & 1) == 0
    return (jnp.where(even, apart, close), jnp.where(even, close, apart))


def matrix_of(kernel):
    width = kernel.shape[-1]
    return jnp.transpose(jnp.flip(kernel, (0, 1)), (0, 3, 1, 2)).reshape(3 * width, 3 * width)


def sum_of_blocks(blocks, axes):
    parts = lax.all_to_all(blocks, axes, 0, 0, tiled=True)
    return jnp.sum(parts.astype(jnp.float32), axis=0)


def copies(block, axes):
    count = lax.axis_size(axes)
    return lax.all_to_all(jnp.broadcast_to(block[None], (count, *block.shape)), axes, 0, 0, tiled=True)


def total_of(x, factor):
    near, stack = (lax.axis_size(NEAR), lax.axis_size("row_0"))
    width = x.shape[-1]
    part = sum_of_blocks(x.reshape(near, -1, width), NEAR).astype(jnp.bfloat16)
    part = part.reshape(stack, 1, -1, width)
    twice = jnp.broadcast_to(part, (stack, lax.axis_size("col_0"), *part.shape[2:]))
    own = sum_of_blocks(twice.reshape(-1, *part.shape[2:]), FAR)
    own = (own * factor).astype(jnp.bfloat16)
    part = copies(own, "row_0").reshape(-1, width)
    return copies(part, NEAR).reshape(x.shape).astype(jnp.float32)


def section_backward(section_input, first_pre, second_pre, out_grad, kernels, bn_scale, bn_shift):
    sections = lax.axis_size("section")
    last = (lax.axis_index("section") == sections - 1).astype(jnp.int32).reshape(1)
    even = ((lax.axis_index(COL) & 1) == 0).astype(jnp.int32).reshape(1)
    micros, rows_here, cols_here, width = out_grad.shape
    bf16 = jnp.bfloat16
    scale = bn_scale[0]
    two = (2, micros, rows_here)
    masks, inward, outward, act, scale = pl.pallas_call(
        prepare_kernel,
        name="prepare",
        in_specs=[SMEM] + [pl.BlockSpec(memory_space=pltpu.MemorySpace.HBM)] * 6,
        out_specs=[VMEM] * 5,
        out_shape=[
            jax.ShapeDtypeStruct((*two, cols_here, width), bf16),
            jax.ShapeDtypeStruct((*two, DEPTH, width), bf16),
            jax.ShapeDtypeStruct((*two, DEPTH, width), bf16),
            jax.ShapeDtypeStruct(out_grad.shape, bf16),
            jax.ShapeDtypeStruct(scale.shape, jnp.float32),
        ],
        scratch_shapes=[
            pltpu.VMEM((4, *out_grad.shape), bf16),
            pltpu.VMEM((2, *scale.shape), jnp.float32),
            pltpu.SemaphoreType.DMA((6,)),
        ],
        compiler_params=PARAMS,
    )(
        jnp.concatenate([last, even]),
        *[
            pltpu.with_memory_space_constraint(x, pltpu.MemorySpace.HBM)
            for x in (section_input[0], first_pre[0], second_pre[0], out_grad, scale, bn_shift[0])
        ],
    )
    left, right = swaps(inward, outward, COL)
    band = jnp.concatenate([left, masks, right], axis=3)
    above, below = swaps(band, band, ROW)
    first = matrix_of(kernels[0, 0])
    second = matrix_of(kernels[0, 1])
    masks = jnp.concatenate([above, band, below], axis=2)
    high, wide = masks.shape[2:4]
    frame = pltpu.VMEM((high, wide, width), jnp.float32)

    received = [[]]
    for step in range(sections - 1):
        reach = 2 * (sections - 1 - step)
        narrow = NARROW if step else 0
        sent = []
        for micro in range(micros):
            taken = [received[-1][micro]] if step else []
            result = pl.pallas_call(
                functools.partial(stage_kernel, micro=micro, reach=reach, narrow=bool(step)),
                in_specs=[VMEM] * (4 + len(taken)),
                out_specs=VMEM,
                out_shape=jax.ShapeDtypeStruct(
                    (rows_here + 2 * reach, wide - 2 * narrow, width), bf16
                ),
                scratch_shapes=[frame],
                compiler_params=PARAMS,
            )(masks, first, second, scale, *taken)
            pair = [(sections - 1 - step, sections - 2 - step)]
            sent.append(lax.ppermute(result, "section", pair))
        received.append(sent)
    frames = pltpu.VMEM((sections - 1, high, wide, width), jnp.float32)
    common = (last, masks, first, second, scale)
    arrived = [[step[micro] for step in received[1:]] for micro in range(micros)]
    ready = []
    for micro in range(micros - 1):
        field = jax.ShapeDtypeStruct((rows_here + 2, wide, width), bf16)
        ready += pl.pallas_call(
            functools.partial(early_kernel, micro=micro),
            in_specs=[SMEM] + [VMEM] * (4 + len(arrived[micro])),
            out_specs=[VMEM] * 3,
            out_shape=[jax.ShapeDtypeStruct(out_grad.shape[1:], bf16), field, field],
            scratch_shapes=[frames],
            compiler_params=PARAMS,
        )(*common, *arrived[micro])
    taken = ready + arrived[-1]
    input_grad, partial = pl.pallas_call(
        functools.partial(last_kernel, micros=micros, early=micros - 1),
        name="last",
        in_specs=[SMEM] + [VMEM] * (6 + len(taken)),
        out_specs=[VMEM] * 2,
        out_shape=[
            jax.ShapeDtypeStruct(out_grad.shape, bf16),
            jax.ShapeDtypeStruct((2, 9, width, width), bf16),
        ],
        scratch_shapes=[frames],
        compiler_params=PARAMS,
    )(*common, section_input[0], act, *taken)
    pixels = micros * rows_here * lax.axis_size(ROW) * cols_here * lax.axis_size(COL)
    factor = 1.0 / jnp.sqrt(jnp.float32(pixels))
    total = total_of(partial, factor).reshape(2, 3, 3, width, width)
    return (input_grad[None], total[None])


def solution(mesh):
    split = Mesh(
        mesh.devices.reshape(mesh.shape["section"], 8, 2, 2, 4),
        ("section", "row_0", "row_1", "col_0", "col_1"),
    )
    in_specs = (
        P("section", None, ROW, COL, None),
        P("section", None, ROW, COL, None),
        P("section", None, ROW, COL, None),
        P(None, ROW, COL, None),
        P("section", None, None, None, None, None),
        P("section", None, None),
        P("section", None, None),
    )
    out_specs = (P("section", None, ROW, COL, None), P("section", None, None, None, None, None))
    return jax.shard_map(
        section_backward, mesh=split, in_specs=in_specs, out_specs=out_specs, check_vma=False
    )
```

```python
import functools

import jax
import jax.numpy as jnp
from jax import lax
from jax.experimental import pallas as pl
from jax.experimental.pallas import tpu as pltpu
from jax.sharding import Mesh
from jax.sharding import PartitionSpec as P

ROW = ("row_0", "row_1")
COL = ("col_0", "col_1")
NEAR = ("row_1", "col_1")
FAR = ("row_0", "col_0")
VMEM = pl.BlockSpec(memory_space=pltpu.VMEM)
SMEM = pl.BlockSpec(memory_space=pltpu.SMEM)
PARAMS = pltpu.CompilerParams(vmem_limit_bytes=24 * 1024 * 1024)


DEPTH = 8
NARROW = 4
PACKED = 2


def prepare_kernel(flags, *refs):
    sources = refs[:6]
    masks, inward, outward, act, kept, fields, norms, done = refs[6:]
    targets = [fields.at[k] for k in range(4)] + [norms.at[k] for k in range(2)]
    moves = [
        pltpu.make_async_copy(source, target, done.at[k])
        for k, (source, target) in enumerate(zip(sources, targets))
    ]
    for move in moves:
        move.start()
    for move in moves:
        move.wait()
    inputs, first_pre, second_pre, out_grad = [fields[k].astype(jnp.float32) for k in range(4)]
    scale, shift = (norms[0], norms[1])
    kept[...] = scale
    width = masks.shape[3]
    first_norm = scale[0] * first_pre + shift[0]
    act[...] = jnp.maximum(first_norm, 0.0).astype(jnp.bfloat16)
    alive = scale[1] * second_pre + shift[1] + inputs > 0
    passing = jnp.where(flags[0] > 0, out_grad, 1.0)
    passed = jnp.where(alive, passing, 0.0)
    on = jnp.where(first_norm > 0, 1.0, 0.0)
    for kind, value in enumerate((passed, on)):
        masks[kind] = value.astype(jnp.bfloat16)
        head = value[:, :, :DEPTH]
        tail = value[:, :, width - DEPTH :]
        inward[kind] = jnp.where(flags[1] > 0, tail, head).astype(jnp.bfloat16)
        outward[kind] = jnp.where(flags[1] > 0, head, tail).astype(jnp.bfloat16)


def correlate(field, kernel):
    rows, cols, width = field.shape
    rows -= 2
    slabs = [field[i : i + rows].reshape(rows * cols, width) for i in range(3)]
    parts = jnp.dot(jnp.concatenate(slabs, axis=1), kernel[...], preferred_element_type=jnp.float32)
    before, here, after = [parts[:, j * width : (j + 1) * width] for j in range(3)]
    total = pltpu.roll(before, 1, 0) + here + pltpu.roll(after, rows * cols - 1, 0)
    return total.reshape(rows, cols, width)


def unit(masks, micro, incoming, first, second, scale, reach):
    top = DEPTH - reach - 2
    rows = masks.shape[2] - 2 * top
    masked = masks[0, micro, top : top + rows].astype(jnp.float32)
    if incoming is not None:
        masked = masked * incoming
    second_grad = (scale[1] * masked).astype(jnp.bfloat16)
    on = masks[1, micro, top + 1 : top + rows - 1].astype(jnp.float32)
    first_grad = (scale[0] * (correlate(second_grad, second) * on)).astype(jnp.bfloat16)
    result = masked[2 : rows - 2] + correlate(first_grad, first)
    return (result, first_grad, second_grad)


def packed(cells, pairs, pack, cut):
    rows, cols, width = cells.shape
    half = rows // 2
    kept = cols - 2 * cut
    pairs[:half] = cells.reshape(half, 2, cols, width)
    for k in range(2):
        pack[:half, k * kept : (k + 1) * kept] = pairs[:half, k, cut : cut + kept]
    return pack[:half]


def unpacked(cells, pairs, pack, skip):
    half = cells.shape[0] - skip
    kept = cells.shape[1] // 2
    cols = pairs.shape[2]
    cut = (cols - kept) // 2
    pack[:half] = cells[skip // 2 : skip // 2 + half].astype(jnp.float32)
    pairs[:half] = jnp.zeros((half, *pairs.shape[1:]), jnp.float32)
    for k in range(2):
        pairs[:half, k, cut : cut + kept] = pack[:half, k * kept : (k + 1) * kept]
    return pairs[:half].reshape(2 * half, cols, pairs.shape[3])


def widened(cells, frame, skip):
    rows = cells.shape[0] - 2 * skip
    value = cells[skip : skip + rows].astype(jnp.float32)
    frame[:rows] = jnp.zeros((rows, *frame.shape[1:]), jnp.float32)
    frame[:rows, NARROW : frame.shape[1] - NARROW] = value
    return frame[:rows]


def stage_kernel(*refs, micro, step, reach):
    active, masks, first, second, scale, *received, out, frame, pairs, pack = refs

    @pl.when(active[0] > 0)
    def _():
        incoming = None
        if step == 1:
            incoming = unpacked(received[0], pairs, pack, 0)
        elif step > 1:
            incoming = widened(received[0], frame, 0)
        result, _, _ = unit(masks, micro, incoming, first, second, scale, reach)
        if step:
            frame[: result.shape[0]] = result
            result = frame[: result.shape[0], NARROW : result.shape[1] - NARROW]
        else:
            result = packed(result, pairs, pack, PACKED)
        out[...] = result.astype(jnp.bfloat16)


def filter_grad(cells, windows):
    spread = []
    for field in windows:
        rows, cols, width = field.shape
        flat = field.astype(jnp.float32).reshape(rows * cols, width)
        turned = (pltpu.roll(flat, rows * cols - 1, 0), flat, pltpu.roll(flat, 1, 0))
        spread.append(
            [
                t.reshape(rows, cols, width)[:, DEPTH : cols - DEPTH].astype(jnp.bfloat16)
                for t in turned
            ]
        )
    height = cells.shape[1]
    width = cells.shape[3]
    sides = []
    for i in range(3):
        for j in range(3):
            parts = [s[j][2 - i : 2 - i + height].reshape(-1, width) for s in spread]
            sides.append(jnp.concatenate(parts, axis=0))
    flat = cells[...].reshape(-1, width)
    side = jnp.concatenate(sides, axis=1)
    return lax.dot_general(
        flat, side, (((0,), (0,)), ((), ())), preferred_element_type=jnp.float32
    )


def settle(last, masks, micro, received, first, second, scale, frame, pairs, pack):
    incoming = jnp.where(last[0] > 0, 1.0, 0.0)
    steps = len(received)
    for step, cells in enumerate(received):
        skip = 2 * (steps - 1 - step)
        if step:
            incoming = incoming + widened(cells, frame.at[step], skip)
        else:
            incoming = incoming + unpacked(cells, pairs, pack, skip)
    result, first_grad, second_grad = unit(masks, micro, incoming, first, second, scale, 0)
    tile = result[:, DEPTH : result.shape[1] - DEPTH].astype(jnp.bfloat16)
    return (tile, first_grad, second_grad[1:-1])


def early_kernel(*refs, micro):
    last, masks, first, second, scale, *received = refs
    *outs, frame, pairs, pack = received[-6:]
    received = received[:-6]
    values = settle(last, masks, micro, received, first, second, scale, frame, pairs, pack)
    for ref, value in zip(outs, values):
        ref[...] = value


def last_kernel(*refs, micros, early):
    last, masks, first, second, scale, inputs, act, *rest = refs
    out, partial, frame, pairs, pack = rest[-5:]
    ready = rest[: 3 * early]
    received = rest[3 * early : -5]
    units = [[ref[...] for ref in ready[3 * m : 3 * m + 3]] for m in range(early)]
    scratch = (frame, pairs, pack)
    units.append(settle(last, masks, micros - 1, received, first, second, scale, *scratch))
    for micro, (tile, _, _) in enumerate(units):
        out[micro] = tile
    width = scale.shape[1]
    for which, cells in enumerate((inputs, act)):
        total = filter_grad(cells, [u[1 + which] for u in units]).astype(jnp.bfloat16)
        for k in range(9):
            partial[which, k] = total[:, k * width : (k + 1) * width]


def swaps(inward, outward, axis):
    count = lax.axis_size(axis)
    crossing = [(i, i + 1) for i in range(1, count - 1, 2)]
    apart = lax.ppermute(outward, axis, crossing + [(j, i) for i, j in crossing])
    close = lax.ppermute(inward, axis, [(i, i ^ 1) for i in range(count)])
    even = (lax.axis_index(axis) & 1) == 0
    return (jnp.where(even, apart, close), jnp.where(even, close, apart))


def matrix_of(kernel):
    width = kernel.shape[-1]
    return jnp.transpose(jnp.flip(kernel, (0, 1)), (0, 3, 1, 2)).reshape(3 * width, 3 * width)


def sum_of_blocks(blocks, axes):
    parts = lax.all_to_all(blocks, axes, 0, 0, tiled=True)
    return jnp.sum(parts.astype(jnp.float32), axis=0)


def copies(block, axes):
    count = lax.axis_size(axes)
    return lax.all_to_all(jnp.broadcast_to(block[None], (count, *block.shape)), axes, 0, 0, tiled=True)


def total_of(x, factor):
    near, stack = (lax.axis_size(NEAR), lax.axis_size("row_0"))
    width = x.shape[-1]
    part = sum_of_blocks(x.reshape(near, -1, width), NEAR).astype(jnp.bfloat16)
    part = part.reshape(stack, 1, -1, width)
    twice = jnp.broadcast_to(part, (stack, lax.axis_size("col_0"), *part.shape[2:]))
    own = sum_of_blocks(twice.reshape(-1, *part.shape[2:]), FAR)
    own = (own * factor).astype(jnp.bfloat16)
    part = copies(own, "row_0").reshape(-1, width)
    return copies(part, NEAR).reshape(x.shape).astype(jnp.float32)


def section_backward(section_input, first_pre, second_pre, out_grad, kernels, bn_scale, bn_shift):
    sections = lax.axis_size("section")
    last = (lax.axis_index("section") == sections - 1).astype(jnp.int32).reshape(1)
    even = ((lax.axis_index(COL) & 1) == 0).astype(jnp.int32).reshape(1)
    micros, rows_here, cols_here, width = out_grad.shape
    bf16 = jnp.bfloat16
    scale = bn_scale[0]
    two = (2, micros, rows_here)
    masks, inward, outward, act, scale = pl.pallas_call(
        prepare_kernel,
        name="prepare",
        in_specs=[SMEM] + [pl.BlockSpec(memory_space=pltpu.MemorySpace.HBM)] * 6,
        out_specs=[VMEM] * 5,
        out_shape=[
            jax.ShapeDtypeStruct((*two, cols_here, width), bf16),
            jax.ShapeDtypeStruct((*two, DEPTH, width), bf16),
            jax.ShapeDtypeStruct((*two, DEPTH, width), bf16),
            jax.ShapeDtypeStruct(out_grad.shape, bf16),
            jax.ShapeDtypeStruct(scale.shape, jnp.float32),
        ],
        scratch_shapes=[
            pltpu.VMEM((4, *out_grad.shape), bf16),
            pltpu.VMEM((2, *scale.shape), jnp.float32),
            pltpu.SemaphoreType.DMA((6,)),
        ],
        compiler_params=PARAMS,
    )(
        jnp.concatenate([last, even]),
        *[
            pltpu.with_memory_space_constraint(x, pltpu.MemorySpace.HBM)
            for x in (section_input[0], first_pre[0], second_pre[0], out_grad, scale, bn_shift[0])
        ],
    )
    left, right = swaps(inward, outward, COL)
    above, below = swaps(masks, masks, ROW)
    sides = jnp.concatenate([left, right], axis=3)
    sides, kernels = lax.optimization_barrier((sides, kernels))
    above_sides, below_sides = swaps(sides, sides, ROW)
    first = matrix_of(kernels[0, 0])
    second = matrix_of(kernels[0, 1])
    bands = [
        jnp.concatenate([side[:, :, :, :DEPTH], middle, side[:, :, :, DEPTH:]], axis=3)
        for side, middle in ((above_sides, above), (sides, masks), (below_sides, below))
    ]
    masks = jnp.concatenate(bands, axis=2)
    high, wide = masks.shape[2:4]
    pairs = [
        pltpu.VMEM((high // 2, 2, wide, width), jnp.float32),
        pltpu.VMEM((high // 2, 2 * (wide - 2 * PACKED), width), jnp.float32),
    ]

    received = [[]]
    for step in range(sections - 1):
        reach = 2 * (sections - 1 - step)
        rows = rows_here + 2 * reach
        shape = (rows, wide - 2 * NARROW, width)
        if step == 0:
            shape = (rows // 2, 2 * (wide - 2 * PACKED), width)
        active = (lax.axis_index("section") == sections - 1 - step).astype(jnp.int32).reshape(1)
        sent = []
        for micro in range(micros):
            taken = [received[-1][micro]] if step else []
            result = pl.pallas_call(
                functools.partial(stage_kernel, micro=micro, step=step, reach=reach),
                in_specs=[SMEM] + [VMEM] * (4 + len(taken)),
                out_specs=VMEM,
                out_shape=jax.ShapeDtypeStruct(shape, bf16),
                scratch_shapes=[pltpu.VMEM((high, wide, width), jnp.float32)] + pairs,
                compiler_params=PARAMS,
            )(active, masks, first, second, scale, *taken)
            pair = [(sections - 1 - step, sections - 2 - step)]
            sent.append(lax.ppermute(result, "section", pair))
        received.append(sent)
    scratch = [pltpu.VMEM((sections - 1, high, wide, width), jnp.float32)] + pairs
    common = (last, masks, first, second, scale)
    arrived = [[step[micro] for step in received[1:]] for micro in range(micros)]
    ready = []
    for micro in range(micros - 1):
        field = jax.ShapeDtypeStruct((rows_here + 2, wide, width), bf16)
        ready += pl.pallas_call(
            functools.partial(early_kernel, micro=micro),
            in_specs=[SMEM] + [VMEM] * (4 + len(arrived[micro])),
            out_specs=[VMEM] * 3,
            out_shape=[jax.ShapeDtypeStruct(out_grad.shape[1:], bf16), field, field],
            scratch_shapes=scratch,
            compiler_params=PARAMS,
        )(*common, *arrived[micro])
    taken = ready + arrived[-1]
    input_grad, partial = pl.pallas_call(
        functools.partial(last_kernel, micros=micros, early=micros - 1),
        name="last",
        in_specs=[SMEM] + [VMEM] * (6 + len(taken)),
        out_specs=[VMEM] * 2,
        out_shape=[
            jax.ShapeDtypeStruct(out_grad.shape, bf16),
            jax.ShapeDtypeStruct((2, 9, width, width), bf16),
        ],
        scratch_shapes=scratch,
        compiler_params=PARAMS,
    )(*common, section_input[0], act, *taken)
    pixels = micros * rows_here * lax.axis_size(ROW) * cols_here * lax.axis_size(COL)
    factor = 1.0 / jnp.sqrt(jnp.float32(pixels))
    total = total_of(partial, factor).reshape(2, 3, 3, width, width)
    return (input_grad[None], total[None])


def solution(mesh):
    split = Mesh(
        mesh.devices.reshape(mesh.shape["section"], 8, 2, 2, 4),
        ("section", "row_0", "row_1", "col_0", "col_1"),
    )
    in_specs = (
        P("section", None, ROW, COL, None),
        P("section", None, ROW, COL, None),
        P("section", None, ROW, COL, None),
        P(None, ROW, COL, None),
        P("section", None, None, None, None, None),
        P("section", None, None),
        P("section", None, None),
    )
    out_specs = (P("section", None, ROW, COL, None), P("section", None, None, None, None, None))
    return jax.shard_map(
        section_backward, mesh=split, in_specs=in_specs, out_specs=out_specs, check_vma=False
    )
```

```python
import functools

import jax
import jax.numpy as jnp
from jax import lax
from jax.experimental import pallas as pl
from jax.experimental.pallas import tpu as pltpu
from jax.sharding import Mesh
from jax.sharding import PartitionSpec as P

ROW = ("row_0", "row_1")
COL = ("col_0", "col_1")
NEAR = ("row_1", "col_1")
FAR = ("row_0", "col_0")
VMEM = pl.BlockSpec(memory_space=pltpu.VMEM)
SMEM = pl.BlockSpec(memory_space=pltpu.SMEM)
PARAMS = pltpu.CompilerParams(vmem_limit_bytes=24 * 1024 * 1024)


DEPTH = 8
NARROW = 4
PACKED = 2


def prepare_kernel(flags, *refs):
    sources = refs[:6]
    masks, inward, outward, act, kept, fields, norms, done = refs[6:]
    targets = [fields.at[k] for k in range(4)] + [norms.at[k] for k in range(2)]
    moves = [
        pltpu.make_async_copy(source, target, done.at[k])
        for k, (source, target) in enumerate(zip(sources, targets))
    ]
    for move in moves:
        move.start()
    for move in moves:
        move.wait()
    inputs, first_pre, second_pre, out_grad = [fields[k].astype(jnp.float32) for k in range(4)]
    scale, shift = (norms[0], norms[1])
    kept[...] = scale
    width = masks.shape[3]
    first_norm = scale[0] * first_pre + shift[0]
    act[...] = jnp.maximum(first_norm, 0.0).astype(jnp.bfloat16)
    alive = scale[1] * second_pre + shift[1] + inputs > 0
    passing = jnp.where(flags[0] > 0, out_grad, 1.0)
    passed = jnp.where(alive, passing, 0.0)
    on = jnp.where(first_norm > 0, 1.0, 0.0)
    for kind, value in enumerate((passed, on)):
        masks[kind] = value.astype(jnp.bfloat16)
        head = value[:, :, :DEPTH]
        tail = value[:, :, width - DEPTH :]
        inward[kind] = jnp.where(flags[1] > 0, tail, head).astype(jnp.bfloat16)
        outward[kind] = jnp.where(flags[1] > 0, head, tail).astype(jnp.bfloat16)


def correlate(field, kernel):
    rows, cols, width = field.shape
    rows -= 2
    slabs = [field[i : i + rows].reshape(rows * cols, width) for i in range(3)]
    parts = jnp.dot(jnp.concatenate(slabs, axis=1), kernel[...], preferred_element_type=jnp.float32)
    before, here, after = [parts[:, j * width : (j + 1) * width] for j in range(3)]
    total = pltpu.roll(before, 1, 0) + here + pltpu.roll(after, rows * cols - 1, 0)
    return total.reshape(rows, cols, width)


def unit(masks, micro, incoming, first, second, scale, reach):
    top = DEPTH - reach - 2
    rows = masks.shape[2] - 2 * top
    masked = masks[0, micro, top : top + rows].astype(jnp.float32)
    if incoming is not None:
        masked = masked * incoming
    second_grad = (scale[1] * masked).astype(jnp.bfloat16)
    on = masks[1, micro, top + 1 : top + rows - 1].astype(jnp.float32)
    first_grad = (scale[0] * (correlate(second_grad, second) * on)).astype(jnp.bfloat16)
    result = masked[2 : rows - 2] + correlate(first_grad, first)
    return (result, first_grad, second_grad)


def packed(cells, pairs, pack, cut):
    rows, cols, width = cells.shape
    half = rows // 2
    kept = cols - 2 * cut
    pairs[:half] = cells.reshape(half, 2, cols, width)
    for k in range(2):
        pack[:half, k * kept : (k + 1) * kept] = pairs[:half, k, cut : cut + kept]
    return pack[:half]


def unpacked(cells, pairs, pack, skip):
    half = cells.shape[0] - skip
    kept = cells.shape[1] // 2
    cols = pairs.shape[2]
    cut = (cols - kept) // 2
    pack[:half] = cells[skip // 2 : skip // 2 + half].astype(jnp.float32)
    pairs[:half] = jnp.zeros((half, *pairs.shape[1:]), jnp.float32)
    for k in range(2):
        pairs[:half, k, cut : cut + kept] = pack[:half, k * kept : (k + 1) * kept]
    return pairs[:half].reshape(2 * half, cols, pairs.shape[3])


def widened(cells, frame, skip):
    rows = cells.shape[0] - 2 * skip
    value = cells[skip : skip + rows].astype(jnp.float32)
    frame[:rows] = jnp.zeros((rows, *frame.shape[1:]), jnp.float32)
    frame[:rows, NARROW : frame.shape[1] - NARROW] = value
    return frame[:rows]


def stage_kernel(*refs, micro, step, reach):
    active, masks, first, second, scale, *received, out, frame, pairs, pack = refs

    @pl.when(active[0] > 0)
    def _():
        incoming = None
        if step == 1:
            incoming = unpacked(received[0], pairs, pack, 0)
        elif step > 1:
            incoming = widened(received[0], frame, 0)
        result, _, _ = unit(masks, micro, incoming, first, second, scale, reach)
        if step:
            frame[: result.shape[0]] = result
            result = frame[: result.shape[0], NARROW : result.shape[1] - NARROW]
        else:
            result = packed(result, pairs, pack, PACKED)
        out[...] = result.astype(jnp.bfloat16)


def filter_grad(cells, windows):
    spread = []
    for field in windows:
        rows, cols, width = field.shape
        flat = field.astype(jnp.float32).reshape(rows * cols, width)
        turned = (pltpu.roll(flat, rows * cols - 1, 0), flat, pltpu.roll(flat, 1, 0))
        spread.append(
            [
                t.reshape(rows, cols, width)[:, DEPTH : cols - DEPTH].astype(jnp.bfloat16)
                for t in turned
            ]
        )
    height = cells.shape[1]
    width = cells.shape[3]
    sides = []
    for i in range(3):
        for j in range(3):
            parts = [s[j][2 - i : 2 - i + height].reshape(-1, width) for s in spread]
            sides.append(jnp.concatenate(parts, axis=0))
    flat = cells[...].reshape(-1, width)
    side = jnp.concatenate(sides, axis=1)
    return lax.dot_general(
        flat, side, (((0,), (0,)), ((), ())), preferred_element_type=jnp.float32
    )


def settle(last, masks, micro, received, first, second, scale, frame, pairs, pack):
    incoming = jnp.where(last[0] > 0, 1.0, 0.0)
    steps = len(received)
    for step, cells in enumerate(received):
        skip = 2 * (steps - 1 - step)
        if step:
            incoming = incoming + widened(cells, frame.at[step], skip)
        else:
            incoming = incoming + unpacked(cells, pairs, pack, skip)
    result, first_grad, second_grad = unit(masks, micro, incoming, first, second, scale, 0)
    tile = result[:, DEPTH : result.shape[1] - DEPTH].astype(jnp.bfloat16)
    return (tile, first_grad, second_grad[1:-1])


def early_kernel(*refs, micro):
    last, masks, first, second, scale, *received = refs
    *outs, frame, pairs, pack = received[-6:]
    received = received[:-6]
    values = settle(last, masks, micro, received, first, second, scale, frame, pairs, pack)
    for ref, value in zip(outs, values):
        ref[...] = value


def last_kernel(*refs, micros, early):
    last, masks, first, second, scale, inputs, act, *rest = refs
    out, partial, frame, pairs, pack = rest[-5:]
    ready = rest[: 3 * early]
    received = rest[3 * early : -5]
    units = [[ref[...] for ref in ready[3 * m : 3 * m + 3]] for m in range(early)]
    scratch = (frame, pairs, pack)
    units.append(settle(last, masks, micros - 1, received, first, second, scale, *scratch))
    for micro, (tile, _, _) in enumerate(units):
        out[micro] = tile
    width = scale.shape[1]
    for which, cells in enumerate((inputs, act)):
        total = filter_grad(cells, [u[1 + which] for u in units]).astype(jnp.bfloat16)
        for k in range(9):
            partial[which, k] = total[:, k * width : (k + 1) * width]


def cross(cells, axis):
    count = lax.axis_size(axis)
    pairs = [(i, i + 1) for i in range(1, count - 1, 2)]
    return lax.ppermute(cells, axis, pairs + [(j, i) for i, j in pairs])


def swap(cells, axis):
    return lax.ppermute(cells, axis, [(i, i ^ 1) for i in range(lax.axis_size(axis))])


def in_place(apart, close, axis):
    even = (lax.axis_index(axis) & 1) == 0
    return (jnp.where(even, apart, close), jnp.where(even, close, apart))


def matrix_of(kernel):
    width = kernel.shape[-1]
    return jnp.transpose(jnp.flip(kernel, (0, 1)), (0, 3, 1, 2)).reshape(3 * width, 3 * width)


def sum_of_blocks(blocks, axes):
    parts = lax.all_to_all(blocks, axes, 0, 0, tiled=True)
    return jnp.sum(parts.astype(jnp.float32), axis=0)


def copies(block, axes):
    count = lax.axis_size(axes)
    return lax.all_to_all(jnp.broadcast_to(block[None], (count, *block.shape)), axes, 0, 0, tiled=True)


def total_of(x, factor):
    near, stack = (lax.axis_size(NEAR), lax.axis_size("row_0"))
    width = x.shape[-1]
    part = sum_of_blocks(x.reshape(near, -1, width), NEAR).astype(jnp.bfloat16)
    part = part.reshape(stack, 1, -1, width)
    twice = jnp.broadcast_to(part, (stack, lax.axis_size("col_0"), *part.shape[2:]))
    own = sum_of_blocks(twice.reshape(-1, *part.shape[2:]), FAR)
    own = (own * factor).astype(jnp.bfloat16)
    part = copies(own, "row_0").reshape(-1, width)
    return copies(part, NEAR).reshape(x.shape).astype(jnp.float32)


def section_backward(section_input, first_pre, second_pre, out_grad, kernels, bn_scale, bn_shift):
    sections = lax.axis_size("section")
    last = (lax.axis_index("section") == sections - 1).astype(jnp.int32).reshape(1)
    even = ((lax.axis_index(COL) & 1) == 0).astype(jnp.int32).reshape(1)
    micros, rows_here, cols_here, width = out_grad.shape
    bf16 = jnp.bfloat16
    scale = bn_scale[0]
    two = (2, micros, rows_here)
    masks, inward, outward, act, scale = pl.pallas_call(
        prepare_kernel,
        name="prepare",
        in_specs=[SMEM] + [pl.BlockSpec(memory_space=pltpu.MemorySpace.HBM)] * 6,
        out_specs=[VMEM] * 5,
        out_shape=[
            jax.ShapeDtypeStruct((*two, cols_here, width), bf16),
            jax.ShapeDtypeStruct((*two, DEPTH, width), bf16),
            jax.ShapeDtypeStruct((*two, DEPTH, width), bf16),
            jax.ShapeDtypeStruct(out_grad.shape, bf16),
            jax.ShapeDtypeStruct(scale.shape, jnp.float32),
        ],
        scratch_shapes=[
            pltpu.VMEM((4, *out_grad.shape), bf16),
            pltpu.VMEM((2, *scale.shape), jnp.float32),
            pltpu.SemaphoreType.DMA((6,)),
        ],
        compiler_params=PARAMS,
    )(
        jnp.concatenate([last, even]),
        *[
            pltpu.with_memory_space_constraint(x, pltpu.MemorySpace.HBM)
            for x in (section_input[0], first_pre[0], second_pre[0], out_grad, scale, bn_shift[0])
        ],
    )
    left, right = in_place(cross(outward, COL), swap(inward, COL), COL)
    middle = cross(masks, ROW)
    sides = jnp.concatenate([left, right], axis=3)
    sides, kernels = lax.optimization_barrier((sides, kernels))
    band = jnp.concatenate([sides[:, :, :, :DEPTH], masks, sides[:, :, :, DEPTH:]], axis=3)
    corners = cross(sides, ROW)
    close = swap(band, ROW)
    first = matrix_of(kernels[0, 0])
    second = matrix_of(kernels[0, 1])
    apart = jnp.concatenate([corners[:, :, :, :DEPTH], middle, corners[:, :, :, DEPTH:]], axis=3)
    above, below = in_place(apart, close, ROW)
    masks = jnp.concatenate([above, band, below], axis=2)
    high, wide = masks.shape[2:4]
    pairs = [
        pltpu.VMEM((high // 2, 2, wide, width), jnp.float32),
        pltpu.VMEM((high // 2, 2 * (wide - 2 * PACKED), width), jnp.float32),
    ]

    received = [[]]
    for step in range(sections - 1):
        reach = 2 * (sections - 1 - step)
        rows = rows_here + 2 * reach
        shape = (rows, wide - 2 * NARROW, width)
        if step == 0:
            shape = (rows // 2, 2 * (wide - 2 * PACKED), width)
        active = (lax.axis_index("section") == sections - 1 - step).astype(jnp.int32).reshape(1)
        sent = []
        for micro in range(micros):
            taken = [received[-1][micro]] if step else []
            result = pl.pallas_call(
                functools.partial(stage_kernel, micro=micro, step=step, reach=reach),
                in_specs=[SMEM] + [VMEM] * (4 + len(taken)),
                out_specs=VMEM,
                out_shape=jax.ShapeDtypeStruct(shape, bf16),
                scratch_shapes=[pltpu.VMEM((high, wide, width), jnp.float32)] + pairs,
                compiler_params=PARAMS,
            )(active, masks, first, second, scale, *taken)
            pair = [(sections - 1 - step, sections - 2 - step)]
            sent.append(lax.ppermute(result, "section", pair))
        received.append(sent)
    scratch = [pltpu.VMEM((sections - 1, high, wide, width), jnp.float32)] + pairs
    common = (last, masks, first, second, scale)
    arrived = [[step[micro] for step in received[1:]] for micro in range(micros)]
    ready = []
    for micro in range(micros - 1):
        field = jax.ShapeDtypeStruct((rows_here + 2, wide, width), bf16)
        ready += pl.pallas_call(
            functools.partial(early_kernel, micro=micro),
            in_specs=[SMEM] + [VMEM] * (4 + len(arrived[micro])),
            out_specs=[VMEM] * 3,
            out_shape=[jax.ShapeDtypeStruct(out_grad.shape[1:], bf16), field, field],
            scratch_shapes=scratch,
            compiler_params=PARAMS,
        )(*common, *arrived[micro])
    taken = ready + arrived[-1]
    input_grad, partial = pl.pallas_call(
        functools.partial(last_kernel, micros=micros, early=micros - 1),
        name="last",
        in_specs=[SMEM] + [VMEM] * (6 + len(taken)),
        out_specs=[VMEM] * 2,
        out_shape=[
            jax.ShapeDtypeStruct(out_grad.shape, bf16),
            jax.ShapeDtypeStruct((2, 9, width, width), bf16),
        ],
        scratch_shapes=scratch,
        compiler_params=PARAMS,
    )(*common, section_input[0], act, *taken)
    pixels = micros * rows_here * lax.axis_size(ROW) * cols_here * lax.axis_size(COL)
    factor = 1.0 / jnp.sqrt(jnp.float32(pixels))
    total = total_of(partial, factor).reshape(2, 3, 3, width, width)
    return (input_grad[None], total[None])


def solution(mesh):
    split = Mesh(
        mesh.devices.reshape(mesh.shape["section"], 8, 2, 2, 4),
        ("section", "row_0", "row_1", "col_0", "col_1"),
    )
    in_specs = (
        P("section", None, ROW, COL, None),
        P("section", None, ROW, COL, None),
        P("section", None, ROW, COL, None),
        P(None, ROW, COL, None),
        P("section", None, None, None, None, None),
        P("section", None, None),
        P("section", None, None),
    )
    out_specs = (P("section", None, ROW, COL, None), P("section", None, None, None, None, None))
    return jax.shard_map(
        section_backward, mesh=split, in_specs=in_specs, out_specs=out_specs, check_vma=False
    )
```

```python
import functools

import jax
import jax.numpy as jnp
from jax import lax
from jax.experimental import pallas as pl
from jax.experimental.pallas import tpu as pltpu
from jax.sharding import Mesh
from jax.sharding import PartitionSpec as P

ROW = ("row_0", "row_1")
COL = ("col_0", "col_1")
NEAR = ("row_1", "col_1")
FAR = ("row_0", "col_0")
VMEM = pl.BlockSpec(memory_space=pltpu.VMEM)
SMEM = pl.BlockSpec(memory_space=pltpu.SMEM)
PARAMS = pltpu.CompilerParams(vmem_limit_bytes=24 * 1024 * 1024)


DEPTH = 8
NARROW = 4
PACKED = 2


def prepare_kernel(flags, *refs):
    sources = refs[:6]
    masks, inward, outward, act, kept, fields, norms, done = refs[6:]
    targets = [fields.at[k] for k in range(4)] + [norms.at[k] for k in range(2)]
    moves = [
        pltpu.make_async_copy(source, target, done.at[k])
        for k, (source, target) in enumerate(zip(sources, targets))
    ]
    for move in moves:
        move.start()
    for move in moves:
        move.wait()
    inputs, first_pre, second_pre, out_grad = [fields[k].astype(jnp.float32) for k in range(4)]
    scale, shift = (norms[0], norms[1])
    kept[...] = scale
    width = masks.shape[3]
    first_norm = scale[0] * first_pre + shift[0]
    act[...] = jnp.maximum(first_norm, 0.0).astype(jnp.bfloat16)
    alive = scale[1] * second_pre + shift[1] + inputs > 0
    passing = jnp.where(flags[0] > 0, out_grad, 1.0)
    passed = jnp.where(alive, passing, 0.0)
    on = jnp.where(first_norm > 0, 1.0, 0.0)
    for kind, value in enumerate((passed, on)):
        masks[kind] = value.astype(jnp.bfloat16)
        head = value[:, :, :DEPTH]
        tail = value[:, :, width - DEPTH :]
        inward[kind] = jnp.where(flags[1] > 0, tail, head).astype(jnp.bfloat16)
        outward[kind] = jnp.where(flags[1] > 0, head, tail).astype(jnp.bfloat16)


def correlate(field, kernel):
    rows, cols, width = field.shape
    rows -= 2
    slabs = [field[i : i + rows].reshape(rows * cols, width) for i in range(3)]
    parts = jnp.dot(jnp.concatenate(slabs, axis=1), kernel[...], preferred_element_type=jnp.float32)
    before, here, after = [parts[:, j * width : (j + 1) * width] for j in range(3)]
    total = pltpu.roll(before, 1, 0) + here + pltpu.roll(after, rows * cols - 1, 0)
    return total.reshape(rows, cols, width)


def unit(masks, micro, incoming, first, second, scale, reach):
    top = DEPTH - reach - 2
    rows = masks.shape[2] - 2 * top
    masked = masks[0, micro, top : top + rows].astype(jnp.float32)
    if incoming is not None:
        masked = masked * incoming
    second_grad = (scale[1] * masked).astype(jnp.bfloat16)
    on = masks[1, micro, top + 1 : top + rows - 1].astype(jnp.float32)
    first_grad = (scale[0] * (correlate(second_grad, second) * on)).astype(jnp.bfloat16)
    result = masked[2 : rows - 2] + correlate(first_grad, first)
    return (result, first_grad, second_grad)


def packed(cells, pairs, pack, cut):
    rows, cols, width = cells.shape
    half = rows // 2
    kept = cols - 2 * cut
    pairs[:half] = cells.reshape(half, 2, cols, width)
    for k in range(2):
        pack[:half, k * kept : (k + 1) * kept] = pairs[:half, k, cut : cut + kept]
    return pack[:half]


def unpacked(cells, pairs, pack, skip):
    half = cells.shape[0] - skip
    kept = cells.shape[1] // 2
    cols = pairs.shape[2]
    cut = (cols - kept) // 2
    pack[:half] = cells[skip // 2 : skip // 2 + half].astype(jnp.float32)
    pairs[:half] = jnp.zeros((half, *pairs.shape[1:]), jnp.float32)
    for k in range(2):
        pairs[:half, k, cut : cut + kept] = pack[:half, k * kept : (k + 1) * kept]
    return pairs[:half].reshape(2 * half, cols, pairs.shape[3])


def widened(cells, frame, skip):
    rows = cells.shape[0] - 2 * skip
    value = cells[skip : skip + rows].astype(jnp.float32)
    frame[:rows] = jnp.zeros((rows, *frame.shape[1:]), jnp.float32)
    frame[:rows, NARROW : frame.shape[1] - NARROW] = value
    return frame[:rows]


def stage_kernel(*refs, micro, step, reach):
    active, masks, first, second, scale, *received, out, frame, pairs, pack = refs

    @pl.when(active[0] > 0)
    def _():
        incoming = None
        if step == 1:
            incoming = unpacked(received[0], pairs, pack, 0)
        elif step > 1:
            incoming = widened(received[0], frame, 0)
        result, _, _ = unit(masks, micro, incoming, first, second, scale, reach)
        if step:
            frame[: result.shape[0]] = result
            result = frame[: result.shape[0], NARROW : result.shape[1] - NARROW]
        else:
            result = packed(result, pairs, pack, PACKED)
        out[...] = result.astype(jnp.bfloat16)


def filter_grad(cells, windows):
    spread = []
    for field in windows:
        rows, cols, width = field.shape
        flat = field.astype(jnp.float32).reshape(rows * cols, width)
        turned = (pltpu.roll(flat, rows * cols - 1, 0), flat, pltpu.roll(flat, 1, 0))
        spread.append(
            [
                t.reshape(rows, cols, width)[:, DEPTH : cols - DEPTH].astype(jnp.bfloat16)
                for t in turned
            ]
        )
    height = cells.shape[1]
    width = cells.shape[3]
    sides = []
    for i in range(3):
        for j in range(3):
            parts = [s[j][2 - i : 2 - i + height].reshape(-1, width) for s in spread]
            sides.append(jnp.concatenate(parts, axis=0))
    flat = cells[...].reshape(-1, width)
    side = jnp.concatenate(sides, axis=1)
    return lax.dot_general(
        flat, side, (((0,), (0,)), ((), ())), preferred_element_type=jnp.float32
    )


def settle(last, masks, micro, received, first, second, scale, frame, pairs, pack):
    incoming = jnp.where(last[0] > 0, 1.0, 0.0)
    steps = len(received)
    for step, cells in enumerate(received):
        skip = 2 * (steps - 1 - step)
        if step:
            incoming = incoming + widened(cells, frame.at[step], skip)
        else:
            incoming = incoming + unpacked(cells, pairs, pack, skip)
    result, first_grad, second_grad = unit(masks, micro, incoming, first, second, scale, 0)
    tile = result[:, DEPTH : result.shape[1] - DEPTH].astype(jnp.bfloat16)
    return (tile, first_grad, second_grad[1:-1])


def early_kernel(*refs, micro):
    last, masks, first, second, scale, *received = refs
    *outs, frame, pairs, pack = received[-6:]
    received = received[:-6]
    values = settle(last, masks, micro, received, first, second, scale, frame, pairs, pack)
    for ref, value in zip(outs, values):
        ref[...] = value


def last_kernel(*refs, micros, early):
    last, masks, first, second, scale, inputs, act, *rest = refs
    out, partial, frame, pairs, pack = rest[-5:]
    ready = rest[: 3 * early]
    received = rest[3 * early : -5]
    units = [[ref[...] for ref in ready[3 * m : 3 * m + 3]] for m in range(early)]
    scratch = (frame, pairs, pack)
    units.append(settle(last, masks, micros - 1, received, first, second, scale, *scratch))
    for micro, (tile, _, _) in enumerate(units):
        out[micro] = tile
    width = scale.shape[1]
    for which, cells in enumerate((inputs, act)):
        total = filter_grad(cells, [u[1 + which] for u in units]).astype(jnp.bfloat16)
        for k in range(9):
            partial[which, k] = total[:, k * width : (k + 1) * width]


def cross(cells, axis):
    count = lax.axis_size(axis)
    pairs = [(i, i + 1) for i in range(1, count - 1, 2)]
    return lax.ppermute(cells, axis, pairs + [(j, i) for i, j in pairs])


def swap(cells, axis):
    return lax.ppermute(cells, axis, [(i, i ^ 1) for i in range(lax.axis_size(axis))])


def in_place(apart, close, axis):
    even = (lax.axis_index(axis) & 1) == 0
    return (jnp.where(even, apart, close), jnp.where(even, close, apart))


def matrix_of(kernel):
    width = kernel.shape[-1]
    return jnp.transpose(jnp.flip(kernel, (0, 1)), (0, 3, 1, 2)).reshape(3 * width, 3 * width)


def sum_of_blocks(blocks, axes):
    parts = lax.all_to_all(blocks, axes, 0, 0, tiled=True)
    return jnp.sum(parts.astype(jnp.float32), axis=0)


def copies(block, axes):
    count = lax.axis_size(axes)
    return lax.all_to_all(jnp.broadcast_to(block[None], (count, *block.shape)), axes, 0, 0, tiled=True)


def write_kernel(first_core, half, other, out, lines, done):
    stack, ring, rows, _ = half.shape
    chunk = stack * rows
    moves = []
    for core in range(2):
        mine = first_core[0] > 0 if core == 0 else first_core[0] == 0
        for x in range(ring):
            start = (core * ring + x) * chunk
            for z in range(stack):
                value = jnp.where(mine, half[z, x].astype(jnp.float32), other[z, x].astype(jnp.float32))
                lines[start + z * rows : start + (z + 1) * rows] = value
            part = pl.ds(start, chunk)
            move = pltpu.make_async_copy(lines.at[part], out.at[part], done.at[len(moves)])
            move.start()
            moves.append(move)
    for move in moves:
        move.wait()


def total_of(x, factor):
    near, stack, ring = (lax.axis_size(NEAR), lax.axis_size("row_0"), lax.axis_size("col_1"))
    width = x.shape[-1]
    part = sum_of_blocks(x.reshape(near, -1, width), NEAR).astype(jnp.bfloat16)
    part = part.reshape(stack, 1, -1, width)
    twice = jnp.broadcast_to(part, (stack, lax.axis_size("col_0"), *part.shape[2:]))
    own = sum_of_blocks(twice.reshape(-1, *part.shape[2:]), FAR)
    own = (own * factor).astype(jnp.bfloat16)
    half = copies(own[None], ("row_0", "col_1"))
    other = lax.ppermute(half, "row_1", [(0, 1), (1, 0)])
    first_core = (lax.axis_index("row_1") == 0).astype(jnp.int32).reshape(1)
    shape = (stack, ring, *own.shape)
    return pl.pallas_call(
        write_kernel,
        name="write",
        in_specs=[SMEM, VMEM, VMEM],
        out_specs=pl.BlockSpec(memory_space=pltpu.MemorySpace.HBM),
        out_shape=jax.ShapeDtypeStruct((x.size // width, width), jnp.float32),
        scratch_shapes=[
            pltpu.VMEM((x.size // width, width), jnp.float32),
            pltpu.SemaphoreType.DMA((2 * ring,)),
        ],
        compiler_params=PARAMS,
    )(first_core, half.reshape(shape), other.reshape(shape))


def section_backward(section_input, first_pre, second_pre, out_grad, kernels, bn_scale, bn_shift):
    sections = lax.axis_size("section")
    last = (lax.axis_index("section") == sections - 1).astype(jnp.int32).reshape(1)
    even = ((lax.axis_index(COL) & 1) == 0).astype(jnp.int32).reshape(1)
    micros, rows_here, cols_here, width = out_grad.shape
    bf16 = jnp.bfloat16
    scale = bn_scale[0]
    two = (2, micros, rows_here)
    masks, inward, outward, act, scale = pl.pallas_call(
        prepare_kernel,
        name="prepare",
        in_specs=[SMEM] + [pl.BlockSpec(memory_space=pltpu.MemorySpace.HBM)] * 6,
        out_specs=[VMEM] * 5,
        out_shape=[
            jax.ShapeDtypeStruct((*two, cols_here, width), bf16),
            jax.ShapeDtypeStruct((*two, DEPTH, width), bf16),
            jax.ShapeDtypeStruct((*two, DEPTH, width), bf16),
            jax.ShapeDtypeStruct(out_grad.shape, bf16),
            jax.ShapeDtypeStruct(scale.shape, jnp.float32),
        ],
        scratch_shapes=[
            pltpu.VMEM((4, *out_grad.shape), bf16),
            pltpu.VMEM((2, *scale.shape), jnp.float32),
            pltpu.SemaphoreType.DMA((6,)),
        ],
        compiler_params=PARAMS,
    )(
        jnp.concatenate([last, even]),
        *[
            pltpu.with_memory_space_constraint(x, pltpu.MemorySpace.HBM)
            for x in (section_input[0], first_pre[0], second_pre[0], out_grad, scale, bn_shift[0])
        ],
    )
    left, right = in_place(cross(outward, COL), swap(inward, COL), COL)
    middle = cross(masks, ROW)
    sides = jnp.concatenate([left, right], axis=3)
    sides, kernels = lax.optimization_barrier((sides, kernels))
    band = jnp.concatenate([sides[:, :, :, :DEPTH], masks, sides[:, :, :, DEPTH:]], axis=3)
    corners = cross(sides, ROW)
    close = swap(band, ROW)
    first = matrix_of(kernels[0, 0])
    second = matrix_of(kernels[0, 1])
    apart = jnp.concatenate([corners[:, :, :, :DEPTH], middle, corners[:, :, :, DEPTH:]], axis=3)
    above, below = in_place(apart, close, ROW)
    masks = jnp.concatenate([above, band, below], axis=2)
    high, wide = masks.shape[2:4]
    pairs = [
        pltpu.VMEM((high // 2, 2, wide, width), jnp.float32),
        pltpu.VMEM((high // 2, 2 * (wide - 2 * PACKED), width), jnp.float32),
    ]

    received = [[]]
    for step in range(sections - 1):
        reach = 2 * (sections - 1 - step)
        rows = rows_here + 2 * reach
        shape = (rows, wide - 2 * NARROW, width)
        if step == 0:
            shape = (rows // 2, 2 * (wide - 2 * PACKED), width)
        active = (lax.axis_index("section") == sections - 1 - step).astype(jnp.int32).reshape(1)
        sent = []
        for micro in range(micros):
            taken = [received[-1][micro]] if step else []
            result = pl.pallas_call(
                functools.partial(stage_kernel, micro=micro, step=step, reach=reach),
                in_specs=[SMEM] + [VMEM] * (4 + len(taken)),
                out_specs=VMEM,
                out_shape=jax.ShapeDtypeStruct(shape, bf16),
                scratch_shapes=[pltpu.VMEM((high, wide, width), jnp.float32)] + pairs,
                compiler_params=PARAMS,
            )(active, masks, first, second, scale, *taken)
            pair = [(sections - 1 - step, sections - 2 - step)]
            sent.append(lax.ppermute(result, "section", pair))
        received.append(sent)
    scratch = [pltpu.VMEM((sections - 1, high, wide, width), jnp.float32)] + pairs
    common = (last, masks, first, second, scale)
    arrived = [[step[micro] for step in received[1:]] for micro in range(micros)]
    ready = []
    for micro in range(micros - 1):
        field = jax.ShapeDtypeStruct((rows_here + 2, wide, width), bf16)
        ready += pl.pallas_call(
            functools.partial(early_kernel, micro=micro),
            in_specs=[SMEM] + [VMEM] * (4 + len(arrived[micro])),
            out_specs=[VMEM] * 3,
            out_shape=[jax.ShapeDtypeStruct(out_grad.shape[1:], bf16), field, field],
            scratch_shapes=scratch,
            compiler_params=PARAMS,
        )(*common, *arrived[micro])
    taken = ready + arrived[-1]
    input_grad, partial = pl.pallas_call(
        functools.partial(last_kernel, micros=micros, early=micros - 1),
        name="last",
        in_specs=[SMEM] + [VMEM] * (6 + len(taken)),
        out_specs=[VMEM] * 2,
        out_shape=[
            jax.ShapeDtypeStruct(out_grad.shape, bf16),
            jax.ShapeDtypeStruct((2, 9, width, width), bf16),
        ],
        scratch_shapes=scratch,
        compiler_params=PARAMS,
    )(*common, section_input[0], act, *taken)
    pixels = micros * rows_here * lax.axis_size(ROW) * cols_here * lax.axis_size(COL)
    factor = 1.0 / jnp.sqrt(jnp.float32(pixels))
    total = total_of(partial, factor).reshape(2, 3, 3, width, width)
    return (input_grad[None], total[None])


def solution(mesh):
    split = Mesh(
        mesh.devices.reshape(mesh.shape["section"], 8, 2, 2, 4),
        ("section", "row_0", "row_1", "col_0", "col_1"),
    )
    in_specs = (
        P("section", None, ROW, COL, None),
        P("section", None, ROW, COL, None),
        P("section", None, ROW, COL, None),
        P(None, ROW, COL, None),
        P("section", None, None, None, None, None),
        P("section", None, None),
        P("section", None, None),
    )
    out_specs = (P("section", None, ROW, COL, None), P("section", None, None, None, None, None))
    return jax.shard_map(
        section_backward, mesh=split, in_specs=in_specs, out_specs=out_specs, check_vma=False
    )
```

```python
import functools

import jax
import jax.numpy as jnp
from jax import lax
from jax.experimental import pallas as pl
from jax.experimental.pallas import tpu as pltpu
from jax.sharding import Mesh
from jax.sharding import PartitionSpec as P

ROW = ("row_0", "row_1")
COL = ("col_0", "col_1")
PLANE = ("row_0", "col_1")
VMEM = pl.BlockSpec(memory_space=pltpu.VMEM)
SMEM = pl.BlockSpec(memory_space=pltpu.SMEM)
PARAMS = pltpu.CompilerParams(vmem_limit_bytes=24 * 1024 * 1024)


DEPTH = 8
NARROW = 4
PACKED = 2


def prepare_kernel(flags, *refs):
    sources = refs[:6]
    masks, inward, outward, act, kept, fields, norms, done = refs[6:]
    targets = [fields.at[k] for k in range(4)] + [norms.at[k] for k in range(2)]
    moves = [
        pltpu.make_async_copy(source, target, done.at[k])
        for k, (source, target) in enumerate(zip(sources, targets))
    ]
    for move in moves:
        move.start()
    for move in moves:
        move.wait()
    inputs, first_pre, second_pre, out_grad = [fields[k].astype(jnp.float32) for k in range(4)]
    scale, shift = (norms[0], norms[1])
    kept[...] = scale
    width = masks.shape[3]
    first_norm = scale[0] * first_pre + shift[0]
    act[...] = jnp.maximum(first_norm, 0.0).astype(jnp.bfloat16)
    alive = scale[1] * second_pre + shift[1] + inputs > 0
    passing = jnp.where(flags[0] > 0, out_grad, 1.0)
    passed = jnp.where(alive, passing, 0.0)
    on = jnp.where(first_norm > 0, 1.0, 0.0)
    for kind, value in enumerate((passed, on)):
        masks[kind] = value.astype(jnp.bfloat16)
        head = value[:, :, :DEPTH]
        tail = value[:, :, width - DEPTH :]
        inward[kind] = jnp.where(flags[1] > 0, tail, head).astype(jnp.bfloat16)
        outward[kind] = jnp.where(flags[1] > 0, head, tail).astype(jnp.bfloat16)


def correlate(field, kernel):
    rows, cols, width = field.shape
    rows -= 2
    slabs = [field[i : i + rows].reshape(rows * cols, width) for i in range(3)]
    parts = jnp.dot(jnp.concatenate(slabs, axis=1), kernel[...], preferred_element_type=jnp.float32)
    before, here, after = [parts[:, j * width : (j + 1) * width] for j in range(3)]
    total = pltpu.roll(before, 1, 0) + here + pltpu.roll(after, rows * cols - 1, 0)
    return total.reshape(rows, cols, width)


def unit(masks, micro, incoming, first, second, scale, reach):
    top = DEPTH - reach - 2
    rows = masks.shape[2] - 2 * top
    masked = masks[0, micro, top : top + rows].astype(jnp.float32)
    if incoming is not None:
        masked = masked * incoming
    second_grad = (scale[1] * masked).astype(jnp.bfloat16)
    on = masks[1, micro, top + 1 : top + rows - 1].astype(jnp.float32)
    first_grad = (scale[0] * (correlate(second_grad, second) * on)).astype(jnp.bfloat16)
    result = masked[2 : rows - 2] + correlate(first_grad, first)
    return (result, first_grad, second_grad)


def packed(cells, pairs, pack, cut):
    rows, cols, width = cells.shape
    half = rows // 2
    kept = cols - 2 * cut
    pairs[:half] = cells.reshape(half, 2, cols, width)
    for k in range(2):
        pack[:half, k * kept : (k + 1) * kept] = pairs[:half, k, cut : cut + kept]
    return pack[:half]


def unpacked(cells, pairs, pack, skip):
    half = cells.shape[0] - skip
    kept = cells.shape[1] // 2
    cols = pairs.shape[2]
    cut = (cols - kept) // 2
    pack[:half] = cells[skip // 2 : skip // 2 + half].astype(jnp.float32)
    pairs[:half] = jnp.zeros((half, *pairs.shape[1:]), jnp.float32)
    for k in range(2):
        pairs[:half, k, cut : cut + kept] = pack[:half, k * kept : (k + 1) * kept]
    return pairs[:half].reshape(2 * half, cols, pairs.shape[3])


def widened(cells, frame, skip):
    rows = cells.shape[0] - 2 * skip
    value = cells[skip : skip + rows].astype(jnp.float32)
    frame[:rows] = jnp.zeros((rows, *frame.shape[1:]), jnp.float32)
    frame[:rows, NARROW : frame.shape[1] - NARROW] = value
    return frame[:rows]


def stage_kernel(*refs, micro, step, reach):
    active, masks, first, second, scale, *received, out, frame, pairs, pack = refs

    @pl.when(active[0] > 0)
    def _():
        incoming = None
        if step == 1:
            incoming = unpacked(received[0], pairs, pack, 0)
        elif step > 1:
            incoming = widened(received[0], frame, 0)
        result, _, _ = unit(masks, micro, incoming, first, second, scale, reach)
        if step:
            frame[: result.shape[0]] = result
            result = frame[: result.shape[0], NARROW : result.shape[1] - NARROW]
        else:
            result = packed(result, pairs, pack, PACKED)
        out[...] = result.astype(jnp.bfloat16)


def filter_grad(cells, windows):
    spread = []
    for field in windows:
        rows, cols, width = field.shape
        flat = field.astype(jnp.float32).reshape(rows * cols, width)
        turned = (pltpu.roll(flat, rows * cols - 1, 0), flat, pltpu.roll(flat, 1, 0))
        spread.append(
            [
                t.reshape(rows, cols, width)[:, DEPTH : cols - DEPTH].astype(jnp.bfloat16)
                for t in turned
            ]
        )
    height = cells.shape[1]
    width = cells.shape[3]
    sides = []
    for i in range(3):
        for j in range(3):
            parts = [s[j][2 - i : 2 - i + height].reshape(-1, width) for s in spread]
            sides.append(jnp.concatenate(parts, axis=0))
    flat = cells[...].reshape(-1, width)
    side = jnp.concatenate(sides, axis=1)
    return lax.dot_general(
        flat, side, (((0,), (0,)), ((), ())), preferred_element_type=jnp.float32
    )


def settle(last, masks, micro, received, first, second, scale, frame, pairs, pack):
    incoming = jnp.where(last[0] > 0, 1.0, 0.0)
    steps = len(received)
    for step, cells in enumerate(received):
        skip = 2 * (steps - 1 - step)
        if step:
            incoming = incoming + widened(cells, frame.at[step], skip)
        else:
            incoming = incoming + unpacked(cells, pairs, pack, skip)
    result, first_grad, second_grad = unit(masks, micro, incoming, first, second, scale, 0)
    tile = result[:, DEPTH : result.shape[1] - DEPTH].astype(jnp.bfloat16)
    return (tile, first_grad, second_grad[1:-1])


def early_kernel(*refs, micro):
    last, masks, first, second, scale, *received = refs
    *outs, frame, pairs, pack = received[-6:]
    received = received[:-6]
    values = settle(last, masks, micro, received, first, second, scale, frame, pairs, pack)
    for ref, value in zip(outs, values):
        ref[...] = value


def last_kernel(*refs, micros, early):
    last, masks, first, second, scale, inputs, act, *rest = refs
    out, keep, give, frame, pairs, pack = rest[-6:]
    ready = rest[: 3 * early]
    received = rest[3 * early : -6]
    units = [[ref[...] for ref in ready[3 * m : 3 * m + 3]] for m in range(early)]
    scratch = (frame, pairs, pack)
    units.append(settle(last, masks, micros - 1, received, first, second, scale, *scratch))
    for micro, (tile, _, _) in enumerate(units):
        out[micro] = tile
    width = scale.shape[1]
    firsts, seconds = [filter_grad(c, [u[1 + k] for u in units]) for k, c in enumerate((inputs, act))]
    for k in range(9):
        part = slice(k * width, (k + 1) * width)
        pair = (firsts[:, part], seconds[:, part])
        keep[k] = jnp.where(last[1] > 0, pair[0], pair[1]).astype(jnp.bfloat16)
        give[k] = jnp.where(last[1] > 0, pair[1], pair[0]).astype(jnp.bfloat16)


def cross(cells, axis):
    count = lax.axis_size(axis)
    pairs = [(i, i + 1) for i in range(1, count - 1, 2)]
    return lax.ppermute(cells, axis, pairs + [(j, i) for i, j in pairs])


def swap(cells, axis):
    return lax.ppermute(cells, axis, [(i, i ^ 1) for i in range(lax.axis_size(axis))])


def in_place(apart, close, axis):
    even = (lax.axis_index(axis) & 1) == 0
    return (jnp.where(even, apart, close), jnp.where(even, close, apart))


def matrix_of(kernel):
    width = kernel.shape[-1]
    return jnp.transpose(jnp.flip(kernel, (0, 1)), (0, 3, 1, 2)).reshape(3 * width, 3 * width)


def sum_of_blocks(blocks, axes):
    parts = lax.all_to_all(blocks, axes, 0, 0, tiled=True)
    return jnp.sum(parts.astype(jnp.float32), axis=0)


def copies(block, axes):
    count = lax.axis_size(axes)
    return lax.all_to_all(jnp.broadcast_to(block[None], (count, *block.shape)), axes, 0, 0, tiled=True)


def write_kernel(first_core, half, other, out, lines, done, *, chunks):
    pieces, rows, _ = half.shape
    size = pieces // chunks * rows
    moves = []
    for core in range(2):
        mine = first_core[0] > 0 if core == 0 else first_core[0] == 0
        for k in range(pieces):
            value = jnp.where(mine, half[k].astype(jnp.float32), other[k].astype(jnp.float32))
            start = (core * pieces + k) * rows
            lines[start : start + rows] = value
            if (start + rows) % size == 0:
                part = pl.ds(start + rows - size, size)
                move = pltpu.make_async_copy(lines.at[part], out.at[part], done.at[len(moves)])
                move.start()
                moves.append(move)
    for move in moves:
        move.wait()


def total_of(keep, give, factor):
    width = keep.shape[-1]
    pieces = lax.axis_size(PLANE)
    swapped = [(0, 1), (1, 0)]
    taken = lax.ppermute(give, "row_1", swapped)
    both = keep.astype(jnp.float32) + taken.astype(jnp.float32)
    blocks = both.astype(jnp.bfloat16).reshape(pieces, -1, width)
    part = sum_of_blocks(blocks, PLANE).astype(jnp.bfloat16)
    beyond = lax.ppermute(part, "col_0", swapped)
    own = (part.astype(jnp.float32) + beyond.astype(jnp.float32)) * factor
    half = copies(own.astype(jnp.bfloat16), PLANE)
    half = half.reshape(pieces, -1, width)
    other = lax.ppermute(half, "row_1", swapped)
    first_core = (lax.axis_index("row_1") == 0).astype(jnp.int32).reshape(1)
    lines = 2 * keep.size // width
    chunks = 4
    return pl.pallas_call(
        functools.partial(write_kernel, chunks=chunks),
        name="write",
        in_specs=[SMEM, VMEM, VMEM],
        out_specs=pl.BlockSpec(memory_space=pltpu.MemorySpace.HBM),
        out_shape=jax.ShapeDtypeStruct((lines, width), jnp.float32),
        scratch_shapes=[
            pltpu.VMEM((lines, width), jnp.float32),
            pltpu.SemaphoreType.DMA((2 * chunks,)),
        ],
        compiler_params=PARAMS,
    )(first_core, half, other)


def section_backward(section_input, first_pre, second_pre, out_grad, kernels, bn_scale, bn_shift):
    sections = lax.axis_size("section")
    last = (lax.axis_index("section") == sections - 1).astype(jnp.int32).reshape(1)
    even = ((lax.axis_index(COL) & 1) == 0).astype(jnp.int32).reshape(1)
    micros, rows_here, cols_here, width = out_grad.shape
    bf16 = jnp.bfloat16
    scale = bn_scale[0]
    two = (2, micros, rows_here)
    masks, inward, outward, act, scale = pl.pallas_call(
        prepare_kernel,
        name="prepare",
        in_specs=[SMEM] + [pl.BlockSpec(memory_space=pltpu.MemorySpace.HBM)] * 6,
        out_specs=[VMEM] * 5,
        out_shape=[
            jax.ShapeDtypeStruct((*two, cols_here, width), bf16),
            jax.ShapeDtypeStruct((*two, DEPTH, width), bf16),
            jax.ShapeDtypeStruct((*two, DEPTH, width), bf16),
            jax.ShapeDtypeStruct(out_grad.shape, bf16),
            jax.ShapeDtypeStruct(scale.shape, jnp.float32),
        ],
        scratch_shapes=[
            pltpu.VMEM((4, *out_grad.shape), bf16),
            pltpu.VMEM((2, *scale.shape), jnp.float32),
            pltpu.SemaphoreType.DMA((6,)),
        ],
        compiler_params=PARAMS,
    )(
        jnp.concatenate([last, even]),
        *[
            pltpu.with_memory_space_constraint(x, pltpu.MemorySpace.HBM)
            for x in (section_input[0], first_pre[0], second_pre[0], out_grad, scale, bn_shift[0])
        ],
    )
    left, right = in_place(cross(outward, COL), swap(inward, COL), COL)
    middle = cross(masks, ROW)
    sides = jnp.concatenate([left, right], axis=3)
    sides, kernels = lax.optimization_barrier((sides, kernels))
    band = jnp.concatenate([sides[:, :, :, :DEPTH], masks, sides[:, :, :, DEPTH:]], axis=3)
    corners = cross(sides, ROW)
    close = swap(band, ROW)
    first = matrix_of(kernels[0, 0])
    second = matrix_of(kernels[0, 1])
    apart = jnp.concatenate([corners[:, :, :, :DEPTH], middle, corners[:, :, :, DEPTH:]], axis=3)
    above, below = in_place(apart, close, ROW)
    masks = jnp.concatenate([above, band, below], axis=2)
    high, wide = masks.shape[2:4]
    pairs = [
        pltpu.VMEM((high // 2, 2, wide, width), jnp.float32),
        pltpu.VMEM((high // 2, 2 * (wide - 2 * PACKED), width), jnp.float32),
    ]

    received = [[]]
    for step in range(sections - 1):
        reach = 2 * (sections - 1 - step)
        rows = rows_here + 2 * reach
        shape = (rows, wide - 2 * NARROW, width)
        if step == 0:
            shape = (rows // 2, 2 * (wide - 2 * PACKED), width)
        active = (lax.axis_index("section") == sections - 1 - step).astype(jnp.int32).reshape(1)
        sent = []
        for micro in range(micros):
            taken = [received[-1][micro]] if step else []
            result = pl.pallas_call(
                functools.partial(stage_kernel, micro=micro, step=step, reach=reach),
                in_specs=[SMEM] + [VMEM] * (4 + len(taken)),
                out_specs=VMEM,
                out_shape=jax.ShapeDtypeStruct(shape, bf16),
                scratch_shapes=[pltpu.VMEM((high, wide, width), jnp.float32)] + pairs,
                compiler_params=PARAMS,
            )(active, masks, first, second, scale, *taken)
            pair = [(sections - 1 - step, sections - 2 - step)]
            sent.append(lax.ppermute(result, "section", pair))
        received.append(sent)
    scratch = [pltpu.VMEM((sections - 1, high, wide, width), jnp.float32)] + pairs
    common = (last, masks, first, second, scale)
    arrived = [[step[micro] for step in received[1:]] for micro in range(micros)]
    ready = []
    for micro in range(micros - 1):
        field = jax.ShapeDtypeStruct((rows_here + 2, wide, width), bf16)
        ready += pl.pallas_call(
            functools.partial(early_kernel, micro=micro),
            in_specs=[SMEM] + [VMEM] * (4 + len(arrived[micro])),
            out_specs=[VMEM] * 3,
            out_shape=[jax.ShapeDtypeStruct(out_grad.shape[1:], bf16), field, field],
            scratch_shapes=scratch,
            compiler_params=PARAMS,
        )(*common, *arrived[micro])
    taken = ready + arrived[-1]
    first_core = (lax.axis_index("row_1") == 0).astype(jnp.int32).reshape(1)
    input_grad, keep, give = pl.pallas_call(
        functools.partial(last_kernel, micros=micros, early=micros - 1),
        name="last",
        in_specs=[SMEM] + [VMEM] * (6 + len(taken)),
        out_specs=[VMEM] * 3,
        out_shape=[
            jax.ShapeDtypeStruct(out_grad.shape, bf16),
            jax.ShapeDtypeStruct((9, width, width), bf16),
            jax.ShapeDtypeStruct((9, width, width), bf16),
        ],
        scratch_shapes=scratch,
        compiler_params=PARAMS,
    )(jnp.concatenate([last, first_core]), *common[1:], section_input[0], act, *taken)
    pixels = micros * rows_here * lax.axis_size(ROW) * cols_here * lax.axis_size(COL)
    factor = 1.0 / jnp.sqrt(jnp.float32(pixels))
    total = total_of(keep, give, factor).reshape(2, 3, 3, width, width)
    return (input_grad[None], total[None])


def solution(mesh):
    split = Mesh(
        mesh.devices.reshape(mesh.shape["section"], 8, 2, 2, 4),
        ("section", "row_0", "row_1", "col_0", "col_1"),
    )
    in_specs = (
        P("section", None, ROW, COL, None),
        P("section", None, ROW, COL, None),
        P("section", None, ROW, COL, None),
        P(None, ROW, COL, None),
        P("section", None, None, None, None, None),
        P("section", None, None),
        P("section", None, None),
    )
    out_specs = (P("section", None, ROW, COL, None), P("section", None, None, None, None, None))
    return jax.shard_map(
        section_backward, mesh=split, in_specs=in_specs, out_specs=out_specs, check_vma=False
    )
```

```python
import functools

import jax
import jax.numpy as jnp
from jax import lax
from jax.experimental import pallas as pl
from jax.experimental.pallas import tpu as pltpu
from jax.sharding import Mesh
from jax.sharding import PartitionSpec as P

ROW = ("row_0", "row_1")
COL = ("col_0", "col_1")
PLANE = ("row_0", "col_0", "col_1")
VMEM = pl.BlockSpec(memory_space=pltpu.VMEM)
SMEM = pl.BlockSpec(memory_space=pltpu.SMEM)
PARAMS = pltpu.CompilerParams(vmem_limit_bytes=24 * 1024 * 1024)


DEPTH = 8
NARROW = 4
PACKED = 2


def prepare_kernel(flags, *refs):
    sources = refs[:6]
    masks, inward, outward, act, kept, fields, norms, done = refs[6:]
    targets = [fields.at[k] for k in range(4)] + [norms.at[k] for k in range(2)]
    moves = [
        pltpu.make_async_copy(source, target, done.at[k])
        for k, (source, target) in enumerate(zip(sources, targets))
    ]
    for move in moves:
        move.start()
    for move in moves:
        move.wait()
    inputs, first_pre, second_pre, out_grad = [fields[k].astype(jnp.float32) for k in range(4)]
    scale, shift = (norms[0], norms[1])
    kept[...] = scale
    width = masks.shape[3]
    first_norm = scale[0] * first_pre + shift[0]
    act[...] = jnp.maximum(first_norm, 0.0).astype(jnp.bfloat16)
    alive = scale[1] * second_pre + shift[1] + inputs > 0
    passing = jnp.where(flags[0] > 0, out_grad, 1.0)
    passed = jnp.where(alive, passing, 0.0)
    on = jnp.where(first_norm > 0, 1.0, 0.0)
    for kind, value in enumerate((passed, on)):
        masks[kind] = value.astype(jnp.bfloat16)
        head = value[:, :, :DEPTH]
        tail = value[:, :, width - DEPTH :]
        inward[kind] = jnp.where(flags[1] > 0, tail, head).astype(jnp.bfloat16)
        outward[kind] = jnp.where(flags[1] > 0, head, tail).astype(jnp.bfloat16)


def correlate(field, kernel):
    rows, cols, width = field.shape
    rows -= 2
    slabs = [field[i : i + rows].reshape(rows * cols, width) for i in range(3)]
    parts = jnp.dot(jnp.concatenate(slabs, axis=1), kernel[...], preferred_element_type=jnp.float32)
    before, here, after = [parts[:, j * width : (j + 1) * width] for j in range(3)]
    total = pltpu.roll(before, 1, 0) + here + pltpu.roll(after, rows * cols - 1, 0)
    return total.reshape(rows, cols, width)


def unit(masks, micro, incoming, first, second, scale, reach):
    top = DEPTH - reach - 2
    rows = masks.shape[2] - 2 * top
    masked = masks[0, micro, top : top + rows].astype(jnp.float32)
    if incoming is not None:
        masked = masked * incoming
    second_grad = (scale[1] * masked).astype(jnp.bfloat16)
    on = masks[1, micro, top + 1 : top + rows - 1].astype(jnp.float32)
    first_grad = (scale[0] * (correlate(second_grad, second) * on)).astype(jnp.bfloat16)
    result = masked[2 : rows - 2] + correlate(first_grad, first)
    return (result, first_grad, second_grad)


def packed(cells, pairs, pack, cut):
    rows, cols, width = cells.shape
    half = rows // 2
    kept = cols - 2 * cut
    pairs[:half] = cells.reshape(half, 2, cols, width)
    for k in range(2):
        pack[:half, k * kept : (k + 1) * kept] = pairs[:half, k, cut : cut + kept]
    return pack[:half]


def unpacked(cells, pairs, pack, skip):
    half = cells.shape[0] - skip
    kept = cells.shape[1] // 2
    cols = pairs.shape[2]
    cut = (cols - kept) // 2
    pack[:half] = cells[skip // 2 : skip // 2 + half].astype(jnp.float32)
    pairs[:half] = jnp.zeros((half, *pairs.shape[1:]), jnp.float32)
    for k in range(2):
        pairs[:half, k, cut : cut + kept] = pack[:half, k * kept : (k + 1) * kept]
    return pairs[:half].reshape(2 * half, cols, pairs.shape[3])


def widened(cells, frame, skip):
    rows = cells.shape[0] - 2 * skip
    value = cells[skip : skip + rows].astype(jnp.float32)
    frame[:rows] = jnp.zeros((rows, *frame.shape[1:]), jnp.float32)
    frame[:rows, NARROW : frame.shape[1] - NARROW] = value
    return frame[:rows]


def stage_kernel(*refs, micro, step, reach):
    active, masks, first, second, scale, *received, out, frame, pairs, pack = refs

    @pl.when(active[0] > 0)
    def _():
        incoming = None
        if step == 1:
            incoming = unpacked(received[0], pairs, pack, 0)
        elif step > 1:
            incoming = widened(received[0], frame, 0)
        result, _, _ = unit(masks, micro, incoming, first, second, scale, reach)
        if step:
            frame[: result.shape[0]] = result
            result = frame[: result.shape[0], NARROW : result.shape[1] - NARROW]
        else:
            result = packed(result, pairs, pack, PACKED)
        out[...] = result.astype(jnp.bfloat16)


def filter_grad(cells, windows):
    spread = []
    for field in windows:
        rows, cols, width = field.shape
        flat = field.astype(jnp.float32).reshape(rows * cols, width)
        turned = (pltpu.roll(flat, rows * cols - 1, 0), flat, pltpu.roll(flat, 1, 0))
        spread.append(
            [
                t.reshape(rows, cols, width)[:, DEPTH : cols - DEPTH].astype(jnp.bfloat16)
                for t in turned
            ]
        )
    height = cells.shape[1]
    width = cells.shape[3]
    sides = []
    for i in range(3):
        for j in range(3):
            parts = [s[j][2 - i : 2 - i + height].reshape(-1, width) for s in spread]
            sides.append(jnp.concatenate(parts, axis=0))
    flat = cells.reshape(-1, width)
    side = jnp.concatenate(sides, axis=1)
    return lax.dot_general(
        flat, side, (((0,), (0,)), ((), ())), preferred_element_type=jnp.float32
    )


def settle(last, masks, micro, received, first, second, scale, frame, pairs, pack):
    incoming = jnp.where(last[0] > 0, 1.0, 0.0)
    steps = len(received)
    for step, cells in enumerate(received):
        skip = 2 * (steps - 1 - step)
        if step:
            incoming = incoming + widened(cells, frame.at[step], skip)
        else:
            incoming = incoming + unpacked(cells, pairs, pack, skip)
    result, first_grad, second_grad = unit(masks, micro, incoming, first, second, scale, 0)
    tile = result[:, DEPTH : result.shape[1] - DEPTH].astype(jnp.bfloat16)
    return (tile, first_grad, second_grad[1:-1])


def early_kernel(*refs, micro):
    last, masks, first, second, scale, *received = refs
    *outs, frame, pairs, pack = received[-6:]
    received = received[:-6]
    values = settle(last, masks, micro, received, first, second, scale, frame, pairs, pack)
    for ref, value in zip(outs, values):
        ref[...] = value


def last_kernel(*refs, micros, early):
    last, masks, first, second, scale, inputs, act, *rest = refs
    out, keep, give, frame, pairs, pack = rest[-6:]
    ready = rest[: 3 * early]
    received = rest[3 * early : -6]
    units = [[ref[...] for ref in ready[3 * m : 3 * m + 3]] for m in range(early)]
    scratch = (frame, pairs, pack)
    units.append(settle(last, masks, micros - 1, received, first, second, scale, *scratch))
    for micro, (tile, _, _) in enumerate(units):
        out[micro] = tile
    width = scale.shape[1]
    wide = jnp.float32
    for out_ref, mine in ((give, last[1] == 0), (keep, last[1] > 0)):
        cells = jnp.where(mine, inputs[...].astype(wide), act[...].astype(wide))
        windows = [jnp.where(mine, u[1].astype(wide), u[2].astype(wide)) for u in units]
        total = filter_grad(cells.astype(jnp.bfloat16), windows).astype(jnp.bfloat16)
        for k in range(9):
            out_ref[k] = total[:, k * width : (k + 1) * width]


def cross(cells, axis):
    count = lax.axis_size(axis)
    pairs = [(i, i + 1) for i in range(1, count - 1, 2)]
    return lax.ppermute(cells, axis, pairs + [(j, i) for i, j in pairs])


def swap(cells, axis):
    return lax.ppermute(cells, axis, [(i, i ^ 1) for i in range(lax.axis_size(axis))])


def in_place(apart, close, axis):
    even = (lax.axis_index(axis) & 1) == 0
    return (jnp.where(even, apart, close), jnp.where(even, close, apart))


def matrix_of(kernel):
    width = kernel.shape[-1]
    return jnp.transpose(jnp.flip(kernel, (0, 1)), (0, 3, 1, 2)).reshape(3 * width, 3 * width)


def sum_of_blocks(blocks, axes):
    parts = lax.all_to_all(blocks, axes, 0, 0, tiled=True)
    return jnp.sum(parts.astype(jnp.float32), axis=0)


def copies(block, axes):
    count = lax.axis_size(axes)
    return lax.all_to_all(jnp.broadcast_to(block[None], (count, *block.shape)), axes, 0, 0, tiled=True)


def write_kernel(first_core, half, other, out, lines, done, *, chunks):
    pieces, rows, _ = half.shape
    size = pieces // chunks * rows
    moves = []
    for core in range(2):
        mine = first_core[0] > 0 if core == 0 else first_core[0] == 0
        for k in range(pieces):
            value = jnp.where(mine, half[k].astype(jnp.float32), other[k].astype(jnp.float32))
            start = (core * pieces + k) * rows
            lines[start : start + rows] = value
            if (start + rows) % size == 0:
                part = pl.ds(start + rows - size, size)
                move = pltpu.make_async_copy(lines.at[part], out.at[part], done.at[len(moves)])
                move.start()
                moves.append(move)
    for move in moves:
        move.wait()


def total_of(keep, give, factor):
    width = keep.shape[-1]
    pieces = lax.axis_size(PLANE)
    swapped = [(0, 1), (1, 0)]
    taken = lax.ppermute(give, "row_1", swapped)
    both = keep.astype(jnp.float32) + taken.astype(jnp.float32)
    blocks = both.astype(jnp.bfloat16).reshape(pieces, -1, width)
    own = sum_of_blocks(blocks, PLANE) * factor
    half = copies(own.astype(jnp.bfloat16), PLANE)
    half = half.reshape(pieces, -1, width)
    other = lax.ppermute(half, "row_1", swapped)
    first_core = (lax.axis_index("row_1") == 0).astype(jnp.int32).reshape(1)
    lines = 2 * keep.size // width
    chunks = 4
    return pl.pallas_call(
        functools.partial(write_kernel, chunks=chunks),
        name="write",
        in_specs=[SMEM, VMEM, VMEM],
        out_specs=pl.BlockSpec(memory_space=pltpu.MemorySpace.HBM),
        out_shape=jax.ShapeDtypeStruct((lines, width), jnp.float32),
        scratch_shapes=[
            pltpu.VMEM((lines, width), jnp.float32),
            pltpu.SemaphoreType.DMA((2 * chunks,)),
        ],
        compiler_params=PARAMS,
    )(first_core, half, other)


def section_backward(section_input, first_pre, second_pre, out_grad, kernels, bn_scale, bn_shift):
    sections = lax.axis_size("section")
    last = (lax.axis_index("section") == sections - 1).astype(jnp.int32).reshape(1)
    even = ((lax.axis_index(COL) & 1) == 0).astype(jnp.int32).reshape(1)
    micros, rows_here, cols_here, width = out_grad.shape
    bf16 = jnp.bfloat16
    scale = bn_scale[0]
    two = (2, micros, rows_here)
    masks, inward, outward, act, scale = pl.pallas_call(
        prepare_kernel,
        name="prepare",
        in_specs=[SMEM] + [pl.BlockSpec(memory_space=pltpu.MemorySpace.HBM)] * 6,
        out_specs=[VMEM] * 5,
        out_shape=[
            jax.ShapeDtypeStruct((*two, cols_here, width), bf16),
            jax.ShapeDtypeStruct((*two, DEPTH, width), bf16),
            jax.ShapeDtypeStruct((*two, DEPTH, width), bf16),
            jax.ShapeDtypeStruct(out_grad.shape, bf16),
            jax.ShapeDtypeStruct(scale.shape, jnp.float32),
        ],
        scratch_shapes=[
            pltpu.VMEM((4, *out_grad.shape), bf16),
            pltpu.VMEM((2, *scale.shape), jnp.float32),
            pltpu.SemaphoreType.DMA((6,)),
        ],
        compiler_params=PARAMS,
    )(
        jnp.concatenate([last, even]),
        *[
            pltpu.with_memory_space_constraint(x, pltpu.MemorySpace.HBM)
            for x in (section_input[0], first_pre[0], second_pre[0], out_grad, scale, bn_shift[0])
        ],
    )
    left, right = in_place(cross(outward, COL), swap(inward, COL), COL)
    middle = cross(masks, ROW)
    sides = jnp.concatenate([left, right], axis=3)
    sides, kernels = lax.optimization_barrier((sides, kernels))
    band = jnp.concatenate([sides[:, :, :, :DEPTH], masks, sides[:, :, :, DEPTH:]], axis=3)
    corners = cross(sides, ROW)
    close = swap(band, ROW)
    first = matrix_of(kernels[0, 0])
    second = matrix_of(kernels[0, 1])
    apart = jnp.concatenate([corners[:, :, :, :DEPTH], middle, corners[:, :, :, DEPTH:]], axis=3)
    above, below = in_place(apart, close, ROW)
    masks = jnp.concatenate([above, band, below], axis=2)
    high, wide = masks.shape[2:4]
    pairs = [
        pltpu.VMEM((high // 2, 2, wide, width), jnp.float32),
        pltpu.VMEM((high // 2, 2 * (wide - 2 * PACKED), width), jnp.float32),
    ]

    received = [[]]
    for step in range(sections - 1):
        reach = 2 * (sections - 1 - step)
        rows = rows_here + 2 * reach
        shape = (rows, wide - 2 * NARROW, width)
        if step == 0:
            shape = (rows // 2, 2 * (wide - 2 * PACKED), width)
        active = (lax.axis_index("section") == sections - 1 - step).astype(jnp.int32).reshape(1)
        sent = []
        for micro in range(micros):
            taken = [received[-1][micro]] if step else []
            result = pl.pallas_call(
                functools.partial(stage_kernel, micro=micro, step=step, reach=reach),
                in_specs=[SMEM] + [VMEM] * (4 + len(taken)),
                out_specs=VMEM,
                out_shape=jax.ShapeDtypeStruct(shape, bf16),
                scratch_shapes=[pltpu.VMEM((high, wide, width), jnp.float32)] + pairs,
                compiler_params=PARAMS,
            )(active, masks, first, second, scale, *taken)
            pair = [(sections - 1 - step, sections - 2 - step)]
            sent.append(lax.ppermute(result, "section", pair))
        received.append(sent)
    scratch = [pltpu.VMEM((sections - 1, high, wide, width), jnp.float32)] + pairs
    common = (last, masks, first, second, scale)
    arrived = [[step[micro] for step in received[1:]] for micro in range(micros)]
    ready = []
    for micro in range(micros - 1):
        field = jax.ShapeDtypeStruct((rows_here + 2, wide, width), bf16)
        ready += pl.pallas_call(
            functools.partial(early_kernel, micro=micro),
            in_specs=[SMEM] + [VMEM] * (4 + len(arrived[micro])),
            out_specs=[VMEM] * 3,
            out_shape=[jax.ShapeDtypeStruct(out_grad.shape[1:], bf16), field, field],
            scratch_shapes=scratch,
            compiler_params=PARAMS,
        )(*common, *arrived[micro])
    taken = ready + arrived[-1]
    first_core = (lax.axis_index("row_1") == 0).astype(jnp.int32).reshape(1)
    input_grad, keep, give = pl.pallas_call(
        functools.partial(last_kernel, micros=micros, early=micros - 1),
        name="last",
        in_specs=[SMEM] + [VMEM] * (6 + len(taken)),
        out_specs=[VMEM] * 3,
        out_shape=[
            jax.ShapeDtypeStruct(out_grad.shape, bf16),
            jax.ShapeDtypeStruct((9, width, width), bf16),
            jax.ShapeDtypeStruct((9, width, width), bf16),
        ],
        scratch_shapes=scratch,
        compiler_params=PARAMS,
    )(jnp.concatenate([last, first_core]), *common[1:], section_input[0], act, *taken)
    pixels = micros * rows_here * lax.axis_size(ROW) * cols_here * lax.axis_size(COL)
    factor = 1.0 / jnp.sqrt(jnp.float32(pixels))
    total = total_of(keep, give, factor).reshape(2, 3, 3, width, width)
    return (input_grad[None], total[None])


def solution(mesh):
    split = Mesh(
        mesh.devices.reshape(mesh.shape["section"], 8, 2, 2, 4),
        ("section", "row_0", "row_1", "col_0", "col_1"),
    )
    in_specs = (
        P("section", None, ROW, COL, None),
        P("section", None, ROW, COL, None),
        P("section", None, ROW, COL, None),
        P(None, ROW, COL, None),
        P("section", None, None, None, None, None),
        P("section", None, None),
        P("section", None, None),
    )
    out_specs = (P("section", None, ROW, COL, None), P("section", None, None, None, None, None))
    return jax.shard_map(
        section_backward, mesh=split, in_specs=in_specs, out_specs=out_specs, check_vma=False
    )
```

```python
import functools

import jax
import jax.numpy as jnp
from jax import lax
from jax.experimental import pallas as pl
from jax.experimental.pallas import tpu as pltpu
from jax.sharding import Mesh
from jax.sharding import PartitionSpec as P

ROW = ("row_0", "row_1")
COL = ("col_0", "col_1")
NEAR = ("row_1", "col_1")
FAR = ("row_0", "col_0")
VMEM = pl.BlockSpec(memory_space=pltpu.VMEM)
SMEM = pl.BlockSpec(memory_space=pltpu.SMEM)
PARAMS = pltpu.CompilerParams(vmem_limit_bytes=24 * 1024 * 1024)


DEPTH = 8
NARROW = 4
PACKED = 2


def prepare_kernel(flags, *refs):
    sources = refs[:6]
    masks, inward, outward, act, kept, fields, norms, done = refs[6:]
    targets = [fields.at[k] for k in range(4)] + [norms.at[k] for k in range(2)]
    moves = [
        pltpu.make_async_copy(source, target, done.at[k])
        for k, (source, target) in enumerate(zip(sources, targets))
    ]
    for move in moves:
        move.start()
    for move in moves:
        move.wait()
    inputs, first_pre, second_pre, out_grad = [fields[k].astype(jnp.float32) for k in range(4)]
    scale, shift = (norms[0], norms[1])
    kept[...] = scale
    width = masks.shape[3]
    first_norm = scale[0] * first_pre + shift[0]
    act[...] = jnp.maximum(first_norm, 0.0).astype(jnp.bfloat16)
    alive = scale[1] * second_pre + shift[1] + inputs > 0
    passing = jnp.where(flags[0] > 0, out_grad, 1.0)
    passed = jnp.where(alive, passing, 0.0)
    on = jnp.where(first_norm > 0, 1.0, 0.0)
    for kind, value in enumerate((passed, on)):
        masks[kind] = value.astype(jnp.bfloat16)
        head = value[:, :, :DEPTH]
        tail = value[:, :, width - DEPTH :]
        inward[kind] = jnp.where(flags[1] > 0, tail, head).astype(jnp.bfloat16)
        outward[kind] = jnp.where(flags[1] > 0, head, tail).astype(jnp.bfloat16)


def correlate(field, kernel):
    rows, cols, width = field.shape
    rows -= 2
    slabs = [field[i : i + rows].reshape(rows * cols, width) for i in range(3)]
    parts = jnp.dot(jnp.concatenate(slabs, axis=1), kernel[...], preferred_element_type=jnp.float32)
    before, here, after = [parts[:, j * width : (j + 1) * width] for j in range(3)]
    total = pltpu.roll(before, 1, 0) + here + pltpu.roll(after, rows * cols - 1, 0)
    return total.reshape(rows, cols, width)


def unit(masks, micro, incoming, first, second, scale, reach):
    top = DEPTH - reach - 2
    rows = masks.shape[2] - 2 * top
    masked = masks[0, micro, top : top + rows].astype(jnp.float32)
    if incoming is not None:
        masked = masked * incoming
    second_grad = (scale[1] * masked).astype(jnp.bfloat16)
    on = masks[1, micro, top + 1 : top + rows - 1].astype(jnp.float32)
    first_grad = (scale[0] * (correlate(second_grad, second) * on)).astype(jnp.bfloat16)
    result = masked[2 : rows - 2] + correlate(first_grad, first)
    return (result, first_grad, second_grad)


def packed(cells, pairs, pack, cut):
    rows, cols, width = cells.shape
    half = rows // 2
    kept = cols - 2 * cut
    pairs[:half] = cells.reshape(half, 2, cols, width)
    for k in range(2):
        pack[:half, k * kept : (k + 1) * kept] = pairs[:half, k, cut : cut + kept]
    return pack[:half]


def unpacked(cells, pairs, pack, skip):
    half = cells.shape[0] - skip
    kept = cells.shape[1] // 2
    cols = pairs.shape[2]
    cut = (cols - kept) // 2
    pack[:half] = cells[skip // 2 : skip // 2 + half].astype(jnp.float32)
    pairs[:half] = jnp.zeros((half, *pairs.shape[1:]), jnp.float32)
    for k in range(2):
        pairs[:half, k, cut : cut + kept] = pack[:half, k * kept : (k + 1) * kept]
    return pairs[:half].reshape(2 * half, cols, pairs.shape[3])


def widened(cells, frame, skip):
    rows = cells.shape[0] - 2 * skip
    value = cells[skip : skip + rows].astype(jnp.float32)
    frame[:rows] = jnp.zeros((rows, *frame.shape[1:]), jnp.float32)
    frame[:rows, NARROW : frame.shape[1] - NARROW] = value
    return frame[:rows]


def stage_kernel(*refs, micro, step, reach):
    active, masks, first, second, scale, *received, out, frame, pairs, pack = refs

    @pl.when(active[0] > 0)
    def _():
        incoming = None
        if step == 1:
            incoming = unpacked(received[0], pairs, pack, 0)
        elif step > 1:
            incoming = widened(received[0], frame, 0)
        result, _, _ = unit(masks, micro, incoming, first, second, scale, reach)
        if step:
            frame[: result.shape[0]] = result
            result = frame[: result.shape[0], NARROW : result.shape[1] - NARROW]
        else:
            result = packed(result, pairs, pack, PACKED)
        out[...] = result.astype(jnp.bfloat16)


def filter_grad(cells, field):
    rows, cols, width = field.shape
    flat = field.astype(jnp.float32).reshape(rows * cols, width)
    turned = (pltpu.roll(flat, rows * cols - 1, 0), flat, pltpu.roll(flat, 1, 0))
    spread = [
        t.reshape(rows, cols, width)[:, DEPTH : cols - DEPTH].astype(jnp.bfloat16) for t in turned
    ]
    height = cells.shape[0]
    sides = [
        spread[j][2 - i : 2 - i + height].reshape(-1, width) for i in range(3) for j in range(3)
    ]
    return lax.dot_general(
        cells.reshape(-1, width),
        jnp.concatenate(sides, axis=1),
        (((0,), (0,)), ((), ())),
        preferred_element_type=jnp.float32,
    )


def settle(last, masks, micro, received, first, second, scale, frame, pairs, pack):
    incoming = jnp.where(last[0] > 0, 1.0, 0.0)
    steps = len(received)
    for step, cells in enumerate(received):
        skip = 2 * (steps - 1 - step)
        if step:
            incoming = incoming + widened(cells, frame.at[step], skip)
        else:
            incoming = incoming + unpacked(cells, pairs, pack, skip)
    result, first_grad, second_grad = unit(masks, micro, incoming, first, second, scale, 0)
    tile = result[:, DEPTH : result.shape[1] - DEPTH].astype(jnp.bfloat16)
    return (tile, first_grad, second_grad[1:-1])


def early_kernel(*refs, micro):
    last, masks, first, second, scale, inputs, act, *received = refs
    tile, sums, frame, pairs, pack = received[-5:]
    received = received[:-5]
    values = settle(last, masks, micro, received, first, second, scale, frame, pairs, pack)
    tile[...] = values[0]
    for which, cells in enumerate((inputs, act)):
        sums[which] = filter_grad(cells[micro], values[1 + which])


def last_kernel(*refs, micros, early):
    last, masks, first, second, scale, inputs, act, *rest = refs
    out, partial, frame, pairs, pack = rest[-5:]
    ready = rest[: 2 * early]
    received = rest[2 * early : -5]
    micro = micros - 1
    values = settle(last, masks, micro, received, first, second, scale, frame, pairs, pack)
    for k in range(early):
        out[k] = ready[2 * k][...]
    out[micro] = values[0]
    width = scale.shape[1]
    for which, cells in enumerate((inputs, act)):
        total = filter_grad(cells[micro], values[1 + which])
        for k in range(early):
            total = total + ready[2 * k + 1][which]
        for k in range(9):
            partial[which, k] = total[:, k * width : (k + 1) * width].astype(jnp.bfloat16)


def cross(cells, axis):
    count = lax.axis_size(axis)
    pairs = [(i, i + 1) for i in range(1, count - 1, 2)]
    return lax.ppermute(cells, axis, pairs + [(j, i) for i, j in pairs])


def swap(cells, axis):
    return lax.ppermute(cells, axis, [(i, i ^ 1) for i in range(lax.axis_size(axis))])


def in_place(apart, close, axis):
    even = (lax.axis_index(axis) & 1) == 0
    return (jnp.where(even, apart, close), jnp.where(even, close, apart))


def matrix_of(kernel):
    width = kernel.shape[-1]
    return jnp.transpose(jnp.flip(kernel, (0, 1)), (0, 3, 1, 2)).reshape(3 * width, 3 * width)


def sum_of_blocks(blocks, axes):
    parts = lax.all_to_all(blocks, axes, 0, 0, tiled=True)
    return jnp.sum(parts.astype(jnp.float32), axis=0)


def copies(block, axes):
    count = lax.axis_size(axes)
    return lax.all_to_all(jnp.broadcast_to(block[None], (count, *block.shape)), axes, 0, 0, tiled=True)


def write_kernel(core, half, *refs):
    out, lines, done = refs[-3:]
    stack, ring, rows, _ = half.shape
    chunk = stack * rows
    base = pl.multiple_of(core[0] * (ring * chunk), chunk)
    moves = []
    for x in range(ring):
        for z in range(stack):
            start = x * chunk + z * rows
            lines[start : start + rows] = half[z, x].astype(jnp.float32)
        source = lines.at[pl.ds(x * chunk, chunk)]
        move = pltpu.make_async_copy(source, out.at[pl.ds(base + x * chunk, chunk)], done.at[x])
        move.start()
        moves.append(move)
    for move in moves:
        move.wait()


def write_half(core, half, before):
    stack, ring, rows, width = half.shape
    lines = stack * ring * rows
    hbm = pl.BlockSpec(memory_space=pltpu.MemorySpace.HBM)
    return pl.pallas_call(
        write_kernel,
        in_specs=[SMEM, VMEM] + [hbm] * len(before),
        out_specs=hbm,
        out_shape=jax.ShapeDtypeStruct((2 * lines, width), jnp.float32),
        input_output_aliases={2: 0} if before else {},
        scratch_shapes=[pltpu.VMEM((lines, width), jnp.float32), pltpu.SemaphoreType.DMA((ring,))],
        compiler_params=PARAMS,
    )(core, half, *before)


def total_of(x, factor):
    near, stack, ring = (lax.axis_size(NEAR), lax.axis_size("row_0"), lax.axis_size("col_1"))
    width = x.shape[-1]
    part = sum_of_blocks(x.reshape(near, -1, width), NEAR).astype(jnp.bfloat16)
    part = part.reshape(stack, 1, -1, width)
    twice = jnp.broadcast_to(part, (stack, lax.axis_size("col_0"), *part.shape[2:]))
    own = sum_of_blocks(twice.reshape(-1, *part.shape[2:]), FAR)
    own = (own * factor).astype(jnp.bfloat16)
    half = copies(own[None], ("row_0", "col_1"))
    half = half.reshape(stack, ring, *own.shape)
    other = lax.ppermute(half, "row_1", [(0, 1), (1, 0)])
    core = lax.axis_index("row_1").astype(jnp.int32).reshape(1)
    written = write_half(core, half, [])
    return write_half(1 - core, other, [written])


def section_backward(section_input, first_pre, second_pre, out_grad, kernels, bn_scale, bn_shift):
    sections = lax.axis_size("section")
    last = (lax.axis_index("section") == sections - 1).astype(jnp.int32).reshape(1)
    even = ((lax.axis_index(COL) & 1) == 0).astype(jnp.int32).reshape(1)
    micros, rows_here, cols_here, width = out_grad.shape
    bf16 = jnp.bfloat16
    scale = bn_scale[0]
    two = (2, micros, rows_here)
    masks, inward, outward, act, scale = pl.pallas_call(
        prepare_kernel,
        name="prepare",
        in_specs=[SMEM] + [pl.BlockSpec(memory_space=pltpu.MemorySpace.HBM)] * 6,
        out_specs=[VMEM] * 5,
        out_shape=[
            jax.ShapeDtypeStruct((*two, cols_here, width), bf16),
            jax.ShapeDtypeStruct((*two, DEPTH, width), bf16),
            jax.ShapeDtypeStruct((*two, DEPTH, width), bf16),
            jax.ShapeDtypeStruct(out_grad.shape, bf16),
            jax.ShapeDtypeStruct(scale.shape, jnp.float32),
        ],
        scratch_shapes=[
            pltpu.VMEM((4, *out_grad.shape), bf16),
            pltpu.VMEM((2, *scale.shape), jnp.float32),
            pltpu.SemaphoreType.DMA((6,)),
        ],
        compiler_params=PARAMS,
    )(
        jnp.concatenate([last, even]),
        *[
            pltpu.with_memory_space_constraint(x, pltpu.MemorySpace.HBM)
            for x in (section_input[0], first_pre[0], second_pre[0], out_grad, scale, bn_shift[0])
        ],
    )
    left, right = in_place(cross(outward, COL), swap(inward, COL), COL)
    middle = cross(masks, ROW)
    sides = jnp.concatenate([left, right], axis=3)
    sides, kernels = lax.optimization_barrier((sides, kernels))
    band = jnp.concatenate([sides[:, :, :, :DEPTH], masks, sides[:, :, :, DEPTH:]], axis=3)
    corners = cross(sides, ROW)
    close = swap(band, ROW)
    first = matrix_of(kernels[0, 0])
    second = matrix_of(kernels[0, 1])
    apart = jnp.concatenate([corners[:, :, :, :DEPTH], middle, corners[:, :, :, DEPTH:]], axis=3)
    above, below = in_place(apart, close, ROW)
    masks = jnp.concatenate([above, band, below], axis=2)
    high, wide = masks.shape[2:4]
    pairs = [
        pltpu.VMEM((high // 2, 2, wide, width), jnp.float32),
        pltpu.VMEM((high // 2, 2 * (wide - 2 * PACKED), width), jnp.float32),
    ]

    received = [[]]
    for step in range(sections - 1):
        reach = 2 * (sections - 1 - step)
        rows = rows_here + 2 * reach
        shape = (rows, wide - 2 * NARROW, width)
        if step == 0:
            shape = (rows // 2, 2 * (wide - 2 * PACKED), width)
        active = (lax.axis_index("section") == sections - 1 - step).astype(jnp.int32).reshape(1)
        sent = []
        for micro in range(micros):
            taken = [received[-1][micro]] if step else []
            result = pl.pallas_call(
                functools.partial(stage_kernel, micro=micro, step=step, reach=reach),
                in_specs=[SMEM] + [VMEM] * (4 + len(taken)),
                out_specs=VMEM,
                out_shape=jax.ShapeDtypeStruct(shape, bf16),
                scratch_shapes=[pltpu.VMEM((high, wide, width), jnp.float32)] + pairs,
                compiler_params=PARAMS,
            )(active, masks, first, second, scale, *taken)
            pair = [(sections - 1 - step, sections - 2 - step)]
            sent.append(lax.ppermute(result, "section", pair))
        received.append(sent)
    scratch = [pltpu.VMEM((sections - 1, high, wide, width), jnp.float32)] + pairs
    common = (last, masks, first, second, scale)
    arrived = [[step[micro] for step in received[1:]] for micro in range(micros)]
    ready = []
    for micro in range(micros - 1):
        sums = jax.ShapeDtypeStruct((2, width, 9 * width), jnp.float32)
        ready += pl.pallas_call(
            functools.partial(early_kernel, micro=micro),
            in_specs=[SMEM] + [VMEM] * (6 + len(arrived[micro])),
            out_specs=[VMEM] * 2,
            out_shape=[jax.ShapeDtypeStruct(out_grad.shape[1:], bf16), sums],
            scratch_shapes=scratch,
            compiler_params=PARAMS,
        )(*common, section_input[0], act, *arrived[micro])
    taken = ready + arrived[-1]
    input_grad, partial = pl.pallas_call(
        functools.partial(last_kernel, micros=micros, early=micros - 1),
        name="last",
        in_specs=[SMEM] + [VMEM] * (6 + len(taken)),
        out_specs=[VMEM] * 2,
        out_shape=[
            jax.ShapeDtypeStruct(out_grad.shape, bf16),
            jax.ShapeDtypeStruct((2, 9, width, width), bf16),
        ],
        scratch_shapes=scratch,
        compiler_params=PARAMS,
    )(*common, section_input[0], act, *taken)
    pixels = micros * rows_here * lax.axis_size(ROW) * cols_here * lax.axis_size(COL)
    factor = 1.0 / jnp.sqrt(jnp.float32(pixels))
    total = total_of(partial, factor).reshape(2, 3, 3, width, width)
    return (input_grad[None], total[None])


def solution(mesh):
    split = Mesh(
        mesh.devices.reshape(mesh.shape["section"], 8, 2, 2, 4),
        ("section", "row_0", "row_1", "col_0", "col_1"),
    )
    in_specs = (
        P("section", None, ROW, COL, None),
        P("section", None, ROW, COL, None),
        P("section", None, ROW, COL, None),
        P(None, ROW, COL, None),
        P("section", None, None, None, None, None),
        P("section", None, None),
        P("section", None, None),
    )
    out_specs = (P("section", None, ROW, COL, None), P("section", None, None, None, None, None))
    return jax.shard_map(
        section_backward, mesh=split, in_specs=in_specs, out_specs=out_specs, check_vma=False
    )
```

```python
import functools

import jax
import jax.numpy as jnp
from jax import lax
from jax.experimental import pallas as pl
from jax.experimental.pallas import tpu as pltpu
from jax.sharding import Mesh
from jax.sharding import PartitionSpec as P

ROW = ("row_0", "row_1")
COL = ("col_0", "col_1")
NEAR = ("row_1", "col_1")
FAR = ("row_0", "col_0")
VMEM = pl.BlockSpec(memory_space=pltpu.VMEM)
SMEM = pl.BlockSpec(memory_space=pltpu.SMEM)
PARAMS = pltpu.CompilerParams(vmem_limit_bytes=24 * 1024 * 1024)


DEPTH = 8
NARROW = 4
PACKED = 2


def prepare_kernel(flags, *refs):
    sources = refs[:6]
    masks, inward, outward, act, kept, fields, norms, done = refs[6:]
    targets = [fields.at[k] for k in range(4)] + [norms.at[k] for k in range(2)]
    moves = [
        pltpu.make_async_copy(source, target, done.at[k])
        for k, (source, target) in enumerate(zip(sources, targets))
    ]
    for move in moves:
        move.start()
    for move in moves:
        move.wait()
    inputs, first_pre, second_pre, out_grad = [fields[k].astype(jnp.float32) for k in range(4)]
    scale, shift = (norms[0], norms[1])
    kept[...] = scale
    width = masks.shape[3]
    first_norm = scale[0] * first_pre + shift[0]
    act[...] = jnp.maximum(first_norm, 0.0).astype(jnp.bfloat16)
    alive = scale[1] * second_pre + shift[1] + inputs > 0
    passing = jnp.where(flags[0] > 0, out_grad, 1.0)
    passed = jnp.where(alive, passing, 0.0)
    on = jnp.where(first_norm > 0, 1.0, 0.0)
    for kind, value in enumerate((passed, on)):
        masks[kind] = value.astype(jnp.bfloat16)
        head = value[:, :, :DEPTH]
        tail = value[:, :, width - DEPTH :]
        inward[kind] = jnp.where(flags[1] > 0, tail, head).astype(jnp.bfloat16)
        outward[kind] = jnp.where(flags[1] > 0, head, tail).astype(jnp.bfloat16)


def correlate(field, kernel):
    rows, cols, width = field.shape
    rows -= 2
    slabs = [field[i : i + rows].reshape(rows * cols, width) for i in range(3)]
    parts = jnp.dot(jnp.concatenate(slabs, axis=1), kernel[...], preferred_element_type=jnp.float32)
    before, here, after = [parts[:, j * width : (j + 1) * width] for j in range(3)]
    total = pltpu.roll(before, 1, 0) + here + pltpu.roll(after, rows * cols - 1, 0)
    return total.reshape(rows, cols, width)


def unit(masks, micro, incoming, first, second, scale, reach):
    top = DEPTH - reach - 2
    rows = masks.shape[2] - 2 * top
    masked = masks[0, micro, top : top + rows].astype(jnp.float32)
    if incoming is not None:
        masked = masked * incoming
    second_grad = (scale[1] * masked).astype(jnp.bfloat16)
    on = masks[1, micro, top + 1 : top + rows - 1].astype(jnp.float32)
    first_grad = (scale[0] * (correlate(second_grad, second) * on)).astype(jnp.bfloat16)
    result = masked[2 : rows - 2] + correlate(first_grad, first)
    return (result, first_grad, second_grad)


def packed(cells, pairs, pack, cut):
    rows, cols, width = cells.shape
    half = rows // 2
    kept = cols - 2 * cut
    pairs[:half] = cells.reshape(half, 2, cols, width)
    for k in range(2):
        pack[:half, k * kept : (k + 1) * kept] = pairs[:half, k, cut : cut + kept]
    return pack[:half, : 2 * kept]


def unpacked(cells, pairs, pack, skip):
    half = cells.shape[0] - skip
    kept = cells.shape[1] // 2
    cols = pairs.shape[2]
    cut = (cols - kept) // 2
    pack[:half, : 2 * kept] = cells[skip // 2 : skip // 2 + half].astype(jnp.float32)
    pairs[:half] = jnp.zeros((half, *pairs.shape[1:]), jnp.float32)
    for k in range(2):
        pairs[:half, k, cut : cut + kept] = pack[:half, k * kept : (k + 1) * kept]
    return pairs[:half].reshape(2 * half, cols, pairs.shape[3])


def widened(cells, frame, skip):
    rows = cells.shape[0] - 2 * skip
    value = cells[skip : skip + rows].astype(jnp.float32)
    frame[:rows] = jnp.zeros((rows, *frame.shape[1:]), jnp.float32)
    frame[:rows, NARROW : frame.shape[1] - NARROW] = value
    return frame[:rows]


def stage_kernel(*refs, micro, step, reach):
    active, masks, first, second, scale, *received, out, frame, pairs, pack = refs

    @pl.when(active[0] > 0)
    def _():
        incoming = None
        if step == 1:
            incoming = unpacked(received[0], pairs, pack, 0)
        elif step > 1:
            incoming = widened(received[0], frame, 0)
        result, _, _ = unit(masks, micro, incoming, first, second, scale, reach)
        if step == 1:
            frame[: result.shape[0]] = result
            result = frame[: result.shape[0], NARROW : result.shape[1] - NARROW]
        else:
            result = packed(result, pairs, pack, PACKED if step == 0 else DEPTH - reach)
        out[...] = result.astype(jnp.bfloat16)


def filter_grad(cells, field):
    rows, cols, width = field.shape
    flat = field.astype(jnp.float32).reshape(rows * cols, width)
    turned = (pltpu.roll(flat, rows * cols - 1, 0), flat, pltpu.roll(flat, 1, 0))
    spread = [
        t.reshape(rows, cols, width)[:, DEPTH : cols - DEPTH].astype(jnp.bfloat16) for t in turned
    ]
    height = cells.shape[0]
    sides = [
        spread[j][2 - i : 2 - i + height].reshape(-1, width) for i in range(3) for j in range(3)
    ]
    return lax.dot_general(
        cells.reshape(-1, width),
        jnp.concatenate(sides, axis=1),
        (((0,), (0,)), ((), ())),
        preferred_element_type=jnp.float32,
    )


def settle(last, masks, micro, received, first, second, scale, frame, pairs, pack):
    incoming = jnp.where(last[0] > 0, 1.0, 0.0)
    steps = len(received)
    for step, cells in enumerate(received):
        skip = 2 * (steps - 1 - step)
        if step == 1:
            incoming = incoming + widened(cells, frame.at[step], skip)
        else:
            incoming = incoming + unpacked(cells, pairs, pack, skip)
    result, first_grad, second_grad = unit(masks, micro, incoming, first, second, scale, 0)
    tile = result[:, DEPTH : result.shape[1] - DEPTH].astype(jnp.bfloat16)
    return (tile, first_grad, second_grad[1:-1])


def early_kernel(*refs, micro):
    last, masks, first, second, scale, inputs, act, *received = refs
    tile, sums, frame, pairs, pack = received[-5:]
    received = received[:-5]
    values = settle(last, masks, micro, received, first, second, scale, frame, pairs, pack)
    tile[...] = values[0]
    for which, cells in enumerate((inputs, act)):
        sums[which] = filter_grad(cells[micro], values[1 + which])


def last_kernel(*refs, micros, early):
    last, masks, first, second, scale, inputs, act, *rest = refs
    out, partial, frame, pairs, pack = rest[-5:]
    ready = rest[: 2 * early]
    received = rest[2 * early : -5]
    micro = micros - 1
    values = settle(last, masks, micro, received, first, second, scale, frame, pairs, pack)
    for k in range(early):
        out[k] = ready[2 * k][...]
    out[micro] = values[0]
    width = scale.shape[1]
    for which, cells in enumerate((inputs, act)):
        total = filter_grad(cells[micro], values[1 + which])
        for k in range(early):
            total = total + ready[2 * k + 1][which]
        for k in range(9):
            partial[which, k] = total[:, k * width : (k + 1) * width].astype(jnp.bfloat16)


def cross(cells, axis):
    count = lax.axis_size(axis)
    pairs = [(i, i + 1) for i in range(1, count - 1, 2)]
    return lax.ppermute(cells, axis, pairs + [(j, i) for i, j in pairs])


def swap(cells, axis):
    return lax.ppermute(cells, axis, [(i, i ^ 1) for i in range(lax.axis_size(axis))])


def in_place(apart, close, axis):
    even = (lax.axis_index(axis) & 1) == 0
    return (jnp.where(even, apart, close), jnp.where(even, close, apart))


def matrix_of(kernel):
    width = kernel.shape[-1]
    return jnp.transpose(jnp.flip(kernel, (0, 1)), (0, 3, 1, 2)).reshape(3 * width, 3 * width)


def sum_of_blocks(blocks, axes):
    parts = lax.all_to_all(blocks, axes, 0, 0, tiled=True)
    return jnp.sum(parts.astype(jnp.float32), axis=0)


def copies(block, axes):
    count = lax.axis_size(axes)
    return lax.all_to_all(jnp.broadcast_to(block[None], (count, *block.shape)), axes, 0, 0, tiled=True)


def write_kernel(core, half, *refs):
    out, lines, done = refs[-3:]
    stack, ring, rows, _ = half.shape
    chunk = stack * rows
    base = pl.multiple_of(core[0] * (ring * chunk), chunk)
    moves = []
    for x in range(ring):
        for z in range(stack):
            start = x * chunk + z * rows
            lines[start : start + rows] = half[z, x].astype(jnp.float32)
        source = lines.at[pl.ds(x * chunk, chunk)]
        move = pltpu.make_async_copy(source, out.at[pl.ds(base + x * chunk, chunk)], done.at[x])
        move.start()
        moves.append(move)
    for move in moves:
        move.wait()


def write_half(core, half, before):
    stack, ring, rows, width = half.shape
    lines = stack * ring * rows
    hbm = pl.BlockSpec(memory_space=pltpu.MemorySpace.HBM)
    return pl.pallas_call(
        write_kernel,
        in_specs=[SMEM, VMEM] + [hbm] * len(before),
        out_specs=hbm,
        out_shape=jax.ShapeDtypeStruct((2 * lines, width), jnp.float32),
        input_output_aliases={2: 0} if before else {},
        scratch_shapes=[pltpu.VMEM((lines, width), jnp.float32), pltpu.SemaphoreType.DMA((ring,))],
        compiler_params=PARAMS,
    )(core, half, *before)


def total_of(x, factor):
    near, stack, ring = (lax.axis_size(NEAR), lax.axis_size("row_0"), lax.axis_size("col_1"))
    width = x.shape[-1]
    part = sum_of_blocks(x.reshape(near, -1, width), NEAR).astype(jnp.bfloat16)
    part = part.reshape(stack, 1, -1, width)
    twice = jnp.broadcast_to(part, (stack, lax.axis_size("col_0"), *part.shape[2:]))
    own = sum_of_blocks(twice.reshape(-1, *part.shape[2:]), FAR)
    own = (own * factor).astype(jnp.bfloat16)
    half = copies(own[None], ("row_0", "col_1"))
    half = half.reshape(stack, ring, *own.shape)
    other = lax.ppermute(half, "row_1", [(0, 1), (1, 0)])
    core = lax.axis_index("row_1").astype(jnp.int32).reshape(1)
    written = write_half(core, half, [])
    return write_half(1 - core, other, [written])


def section_backward(section_input, first_pre, second_pre, out_grad, kernels, bn_scale, bn_shift):
    sections = lax.axis_size("section")
    last = (lax.axis_index("section") == sections - 1).astype(jnp.int32).reshape(1)
    even = ((lax.axis_index(COL) & 1) == 0).astype(jnp.int32).reshape(1)
    micros, rows_here, cols_here, width = out_grad.shape
    bf16 = jnp.bfloat16
    scale = bn_scale[0]
    two = (2, micros, rows_here)
    masks, inward, outward, act, scale = pl.pallas_call(
        prepare_kernel,
        name="prepare",
        in_specs=[SMEM] + [pl.BlockSpec(memory_space=pltpu.MemorySpace.HBM)] * 6,
        out_specs=[VMEM] * 5,
        out_shape=[
            jax.ShapeDtypeStruct((*two, cols_here, width), bf16),
            jax.ShapeDtypeStruct((*two, DEPTH, width), bf16),
            jax.ShapeDtypeStruct((*two, DEPTH, width), bf16),
            jax.ShapeDtypeStruct(out_grad.shape, bf16),
            jax.ShapeDtypeStruct(scale.shape, jnp.float32),
        ],
        scratch_shapes=[
            pltpu.VMEM((4, *out_grad.shape), bf16),
            pltpu.VMEM((2, *scale.shape), jnp.float32),
            pltpu.SemaphoreType.DMA((6,)),
        ],
        compiler_params=PARAMS,
    )(
        jnp.concatenate([last, even]),
        *[
            pltpu.with_memory_space_constraint(x, pltpu.MemorySpace.HBM)
            for x in (section_input[0], first_pre[0], second_pre[0], out_grad, scale, bn_shift[0])
        ],
    )
    left, right = in_place(cross(outward, COL), swap(inward, COL), COL)
    middle = cross(masks, ROW)
    sides = jnp.concatenate([left, right], axis=3)
    sides, kernels = lax.optimization_barrier((sides, kernels))
    band = jnp.concatenate([sides[:, :, :, :DEPTH], masks, sides[:, :, :, DEPTH:]], axis=3)
    corners = cross(sides, ROW)
    close = swap(band, ROW)
    first = matrix_of(kernels[0, 0])
    second = matrix_of(kernels[0, 1])
    apart = jnp.concatenate([corners[:, :, :, :DEPTH], middle, corners[:, :, :, DEPTH:]], axis=3)
    above, below = in_place(apart, close, ROW)
    masks = jnp.concatenate([above, band, below], axis=2)
    high, wide = masks.shape[2:4]
    pairs = [
        pltpu.VMEM((high // 2, 2, wide, width), jnp.float32),
        pltpu.VMEM((high // 2, 2 * (wide - 2 * PACKED), width), jnp.float32),
    ]

    received = [[]]
    for step in range(sections - 1):
        reach = 2 * (sections - 1 - step)
        rows = rows_here + 2 * reach
        shape = (rows, wide - 2 * NARROW, width)
        if step == 0:
            shape = (rows // 2, 2 * (wide - 2 * PACKED), width)
        elif step == 2:
            shape = (rows // 2, 2 * (wide - 2 * (DEPTH - reach)), width)
        active = (lax.axis_index("section") == sections - 1 - step).astype(jnp.int32).reshape(1)
        sent = []
        for micro in range(micros):
            taken = [received[-1][micro]] if step else []
            result = pl.pallas_call(
                functools.partial(stage_kernel, micro=micro, step=step, reach=reach),
                in_specs=[SMEM] + [VMEM] * (4 + len(taken)),
                out_specs=VMEM,
                out_shape=jax.ShapeDtypeStruct(shape, bf16),
                scratch_shapes=[pltpu.VMEM((high, wide, width), jnp.float32)] + pairs,
                compiler_params=PARAMS,
            )(active, masks, first, second, scale, *taken)
            pair = [(sections - 1 - step, sections - 2 - step)]
            sent.append(lax.ppermute(result, "section", pair))
        received.append(sent)
    scratch = [pltpu.VMEM((sections - 1, high, wide, width), jnp.float32)] + pairs
    common = (last, masks, first, second, scale)
    arrived = [[step[micro] for step in received[1:]] for micro in range(micros)]
    ready = []
    for micro in range(micros - 1):
        sums = jax.ShapeDtypeStruct((2, width, 9 * width), jnp.float32)
        ready += pl.pallas_call(
            functools.partial(early_kernel, micro=micro),
            in_specs=[SMEM] + [VMEM] * (6 + len(arrived[micro])),
            out_specs=[VMEM] * 2,
            out_shape=[jax.ShapeDtypeStruct(out_grad.shape[1:], bf16), sums],
            scratch_shapes=scratch,
            compiler_params=PARAMS,
        )(*common, section_input[0], act, *arrived[micro])
    taken = ready + arrived[-1]
    input_grad, partial = pl.pallas_call(
        functools.partial(last_kernel, micros=micros, early=micros - 1),
        name="last",
        in_specs=[SMEM] + [VMEM] * (6 + len(taken)),
        out_specs=[VMEM] * 2,
        out_shape=[
            jax.ShapeDtypeStruct(out_grad.shape, bf16),
            jax.ShapeDtypeStruct((2, 9, width, width), bf16),
        ],
        scratch_shapes=scratch,
        compiler_params=PARAMS,
    )(*common, section_input[0], act, *taken)
    pixels = micros * rows_here * lax.axis_size(ROW) * cols_here * lax.axis_size(COL)
    factor = 1.0 / jnp.sqrt(jnp.float32(pixels))
    total = total_of(partial, factor).reshape(2, 3, 3, width, width)
    return (input_grad[None], total[None])


def solution(mesh):
    split = Mesh(
        mesh.devices.reshape(mesh.shape["section"], 8, 2, 2, 4),
        ("section", "row_0", "row_1", "col_0", "col_1"),
    )
    in_specs = (
        P("section", None, ROW, COL, None),
        P("section", None, ROW, COL, None),
        P("section", None, ROW, COL, None),
        P(None, ROW, COL, None),
        P("section", None, None, None, None, None),
        P("section", None, None),
        P("section", None, None),
    )
    out_specs = (P("section", None, ROW, COL, None), P("section", None, None, None, None, None))
    return jax.shard_map(
        section_backward, mesh=split, in_specs=in_specs, out_specs=out_specs, check_vma=False
    )
```
